32 devices in a mesh: dp: 8 (over z, x), mp: 4 (over y, core).
Axes of the slice: x: 2, y: 2, z: 4, core: 2. Of those that a mesh axis runs over, the one named last changes fastest.
Arguments:
- stats: float32 [4, 64, 256, 256], P('mp', 'dp'), may hold values from -1 to 1, as said below
- prev_roots: float32 [4, 64, 256, 256], P('mp', 'dp'), may hold values from -1 to 2, as said below
- counts: int32 [4, 8], replicated, may hold values from 1 to 8, as said below
- grads: bfloat16 [4, 64, 256, 1024], P(None, 'dp', None, 'mp'), may hold values from -6 to 6
Outputs:
- precond: bfloat16 [4, 64, 256, 1024], P(None, 'dp', None, 'mp')
The draws below stay inside these ranges and needn't reach their ends.
Inputs may be any that keep to these rules, and one draw needn't show every extreme that they name: Each model shard's live blocks are the first count slots of each of its devices; every count is 1 to 8, 8 is reached on some device, and the counts of one model shard sum to at most 32, which some model shard reaches. `stats`: every block is symmetric positive definite. `prev_roots`: every block is symmetric.
All inputs are finite; a program needn't handle non-finite values.
Results may differ from the reference program's by a relative error of at most 0.0052.
Values may be sent and summed in bfloat16 or wider, within the bound.
A program may use at most 128 MiB of HBM per device.

```python
import math
import jax
import jax.numpy as jnp
from jax import lax

B = 256
NEWTON = 2
SLOT = 8
SHARE = 4
OWNERS = 4
WORKERS = 8


def symmetric_noise(noise_key, block_shape, spread):
    values = jnp.clip(jax.random.normal(noise_key, block_shape, jnp.float32), -4.0, 4.0)
    return (values + jnp.swapaxes(values, -1, -2)) * (spread / math.sqrt(2.0 * B))


def draw_stats(key, part):
    block_shape = (OWNERS, WORKERS * SLOT, B, B)
    first_key, second_key = jax.random.split(jax.random.fold_in(key, 101))
    noise_part = symmetric_noise(first_key, block_shape, 0.25)
    scales = jnp.exp(jax.random.uniform(second_key, block_shape[:-1], jnp.float32, math.log(0.8), math.log(1.25)))
    identity = jnp.eye(B, dtype=jnp.float32)
    return 0.4 * scales[..., :, None] * (identity + noise_part) * scales[..., None, :]


def draw_prev_roots(key, part):
    block_shape = (OWNERS, WORKERS * SLOT, B, B)
    noise_part = symmetric_noise(jax.random.fold_in(key, 202), block_shape, 0.2)
    return jnp.eye(B, dtype=jnp.float32) + noise_part


def draw_counts(key, part):
    key_list = jax.random.split(jax.random.fold_in(key, 303), 4)
    spare_units = (SHARE - 1) * WORKERS
    full_row = jax.random.randint(key_list[0], (), 0, OWNERS)
    extra_units = jax.random.randint(key_list[1], (OWNERS,), 3 * spare_units // 4, spare_units + 1)
    is_full = jnp.arange(OWNERS) == full_row
    extra_units = jnp.where(is_full, spare_units, extra_units)
    favoured = jax.random.randint(key_list[2], (OWNERS,), 0, WORKERS)
    unit_count = WORKERS * (SLOT - 1)
    scores = jax.random.randint(key_list[3], (OWNERS, WORKERS, SLOT - 1), 0, 65536)
    position = jnp.arange(unit_count, dtype=jnp.int32).reshape(1, WORKERS, SLOT - 1)
    boosted = (jnp.arange(WORKERS)[None, :, None] == favoured[:, None, None]) & is_full[:, None, None]
    scores = scores * unit_count + position + boosted.astype(jnp.int32) * (65536 * unit_count)
    flat_scores = scores.reshape(OWNERS, unit_count)
    ordering = jnp.argsort(-flat_scores, axis=1)
    unit_rank = jnp.argsort(ordering, axis=1)
    chosen = (unit_rank < extra_units[:, None]).astype(jnp.int32).reshape(OWNERS, WORKERS, SLOT - 1)
    return (1 + jnp.sum(chosen, axis=2)).astype(jnp.int32)


def levels(stream_key, extent, shards, least, largest):
    loudness = 1.0
    for axis_at, parts in shards:
        heights = jax.random.uniform(jax.random.fold_in(jax.random.fold_in(stream_key, 6), axis_at), (parts,), jnp.float32, least / len(shards), largest / len(shards))
        loudness = loudness * jnp.repeat(jnp.exp(heights), extent[axis_at] // parts).reshape((-1,) + (1,) * (len(extent) - 1 - axis_at))
    return loudness


def bell_draw(rng, extent, scale, reach, shards=(), kind=jnp.bfloat16):
    values = jax.random.normal(rng, extent, jnp.float32) * scale
    if len(shards) > 0:
        values = levels(rng, extent, shards, -0.22, 0.18) * values
    return jnp.clip(values, min=-reach, max=reach).astype(kind)


def setup_inputs(seed: int = 0) -> dict:
    seeds = jax.random.split(jax.random.key(seed), 5)
    stats = draw_stats(jax.random.fold_in(seeds[4], 71), 0)
    prev_roots = draw_prev_roots(jax.random.fold_in(seeds[4], 71), 0)
    counts = draw_counts(jax.random.fold_in(seeds[4], 71), 0)
    grads = bell_draw(seeds[3], (OWNERS, WORKERS * SLOT, B, OWNERS * B), 1.0, 6.0, ((1, 8), (3, 4)))
    return dict(stats=stats, prev_roots=prev_roots, counts=counts, grads=grads)


def product(left_side, right_side):
    return jnp.einsum("nij,njk->nik", left_side, right_side, precision=lax.Precision.HIGHEST)


def newton_root(statistic, initial):
    identity = jnp.eye(statistic.shape[-1], dtype=statistic.dtype)
    square = product(initial, initial)
    moment = product(product(square, square), statistic)
    estimate = initial
    for iteration in range(NEWTON):
        newton_step = (5.0 * identity - moment) * 0.25
        estimate = product(estimate, newton_step)
        if iteration + 1 < NEWTON:
            double = product(newton_step, newton_step)
            moment = product(product(double, double), moment)
    return estimate


def precondition_owner(paired):
    left_side = paired[0].astype(jnp.float32)
    right_side = paired[1].astype(jnp.float32)
    return jnp.einsum("gab,gbc->gac", left_side, right_side).astype(jnp.bfloat16)


def reference(stats, prev_roots, counts, grads):
    block_groups = OWNERS * WORKERS
    grouped = (stats.reshape(block_groups, SLOT, B, B), prev_roots.reshape(block_groups, SLOT, B, B))
    root_blocks = lax.map(lambda paired: newton_root(paired[0], paired[1]), grouped)
    live_mask = jnp.arange(SLOT, dtype=jnp.int32)[None, None, :] < counts[:, :, None]
    live_mask = live_mask.reshape(block_groups, SLOT, 1, 1)
    band_root = jnp.where(live_mask, root_blocks.astype(jnp.bfloat16), jnp.zeros((), jnp.bfloat16))
    band_root = band_root.reshape(OWNERS, WORKERS * SLOT, B, B)
    return lax.map(precondition_owner, (band_root, grads))
```

```python
import functools

import jax
import jax.numpy as jnp
from jax import lax
from jax.experimental import pallas as pl
from jax.experimental.pallas import tpu as pltpu
from jax.sharding import PartitionSpec as P

VMEM_BYTES = 67043328 - 65536
MESH = pl.DeviceIdType.MESH
RELAYS = 3
WINDOW = 3


def dot(left, right):
    return jnp.dot(left.astype(jnp.bfloat16), right.astype(jnp.bfloat16), preferred_element_type=jnp.float32)


def shifted_squares(parts):
    return [2.0 * part + dot(part, part) for part in parts]


def newton_roots(statistics, initials):
    size = initials[0].shape[-1]
    rows = lax.broadcasted_iota(jnp.int32, (size, size), 0)
    columns = lax.broadcasted_iota(jnp.int32, (size, size), 1)
    identity = jnp.where(rows == columns, 1.0, 0.0).astype(jnp.float32)
    fourths = shifted_squares(shifted_squares([initial - identity for initial in initials]))
    moments = [statistic + dot(fourth, statistic) for fourth, statistic in zip(fourths, statistics)]
    changes = [0.25 * (identity - moment) for moment in moments]
    estimates = [initial + dot(initial, change) for initial, change in zip(initials, changes)]
    fourths = shifted_squares(shifted_squares(changes))
    moments = [moment + dot(fourth, moment) for fourth, moment in zip(fourths, moments)]
    changes = [0.25 * (identity - moment) for moment in moments]
    return [estimate + dot(estimate, change) for estimate, change in zip(estimates, changes)]


def packed_at(index, first, second, slots):
    both = jnp.minimum(first, second)
    paired = index < 2 * both
    slot = jnp.where(paired, lax.div(index, 2), index - both)
    core = jnp.where(paired, lax.rem(index, 2), jnp.where(first > second, 0, 1))
    return core, jnp.clip(slot, 0, slots - 1)


def neighbour_of(data):
    return data + 1 - 2 * lax.rem(data, 2)


def relayed_block(number):
    return number % 2, 1 + number // 2


class Load:
    def __init__(self, counts, chip, data, positions):
        self.first, self.second = counts[2 * chip, data], counts[2 * chip + 1, data]
        self.excess = jnp.maximum(self.first + self.second - positions, 0)


def choosing_kernel(sizes, relays, counts, choice):
    members, workers = counts.shape
    need = jnp.int32(0)
    for chip in range(members // 2):
        for data in range(0, workers, 2):
            pair = [counts[2 * chip, at] + counts[2 * chip + 1, at] for at in (data, data + 1)]
            need = jnp.maximum(need, lax.div(pair[0] + pair[1] + 1, 2))
            need = jnp.maximum(need, jnp.maximum(*pair) - relays)
    choice[0] = sum((need > size).astype(jnp.int32) for size in sizes[:-1])


def kernel(members, positions, relays, window, count_table, stats, starts, grads, near, far, counts, count_sem,
           a_buf, x_buf, g_buf, pool, staged, landed, relayed, returned, a_sem, x_sem, g_sem, y_send, y_recv, p_send, p_recv,
           f_send, f_recv, r_send, r_recv, b_send, b_recv, h_send, h_recv):
    me = lax.axis_index("mp")
    data = lax.axis_index("dp")
    slots, size = stats.shape[1], stats.shape[2]
    chips = members // 2
    core = lax.rem(me, 2)
    chip = me // 2
    other = 1 - core
    partner = 2 * chip + other
    beside = neighbour_of(data)
    half = size // 2
    group = 4

    def rows_of(which):
        return pl.ds(pl.multiple_of(which * half, half), half)

    def peer(offset):
        return lax.rem(chip + offset, chips) * 2 + core

    def source_of(offset):
        return lax.rem(chip + chips - offset, chips)

    def a_copy(slot):
        return pltpu.make_async_copy(stats.at[0, slot], a_buf.at[slot], a_sem.at[slot])

    def x_copy(slot):
        return pltpu.make_async_copy(starts.at[0, slot], x_buf.at[slot], x_sem.at[slot])

    def g_copy(owner):
        return pltpu.make_async_copy(grads.at[owner], g_buf.at[owner], g_sem.at[owner])

    def send(source, place, target, send_sem, recv_sem):
        return pltpu.make_async_remote_copy(
            src_ref=source, dst_ref=place, send_sem=send_sem, recv_sem=recv_sem,
            device_id=target, device_id_type=MESH)

    def p_copy(which, slot):
        block = pool.at[which, slot]
        return send(block, block, {"mp": partner}, p_send.at[slot], p_recv.at[slot])

    def first_copy(offset):
        return send(pool.at[core, 0], landed.at[offset - 1, core], {"mp": peer(offset)},
                    y_send.at[offset - 1, 0], y_recv.at[offset - 1, 0])

    def first_forward(offset, which):
        block = landed.at[offset - 1, which]
        return send(block, block, {"mp": partner}, f_send.at[offset - 1, 0], f_recv.at[offset - 1, 0])

    def y_copy(offset, position):
        return send(staged.at[position - 2], landed.at[offset - 1, position, rows_of(core)], {"mp": peer(offset)},
                    y_send.at[offset - 1, position - 1], y_recv.at[offset - 1, position - 1])

    def forward(offset, position, which):
        block = landed.at[offset - 1, position, rows_of(which)]
        return send(block, block, {"mp": partner}, f_send.at[offset - 1, position - 1], f_recv.at[offset - 1, position - 1])

    def relay_copy(number, which):
        at_core, at_slot = relayed_block(number)
        return send(pool.at[at_core, at_slot, rows_of(which)], relayed.at[number], {"dp": beside, "mp": 2 * chip + which},
                    r_send.at[number, which], r_recv.at[number])

    def back_copy(offset, number):
        return send(landed.at[offset - 1, window + number, rows_of(core)], returned.at[offset - 1, number, rows_of(core)],
                    {"dp": beside, "mp": me}, b_send.at[offset - 1, number], b_recv.at[offset - 1, number])

    def back_forward(offset, number, which):
        block = returned.at[offset - 1, number, rows_of(which)]
        return send(block, block, {"mp": partner}, h_send.at[offset - 1, number], h_recv.at[offset - 1, number])

    count_copy = pltpu.make_async_copy(count_table, counts, count_sem)
    for slot in range(group):
        x_copy(slot).start()
    for slot in range(group):
        a_copy(slot).start()
    count_copy.start()

    barrier = pltpu.get_barrier_semaphore()
    pl.semaphore_signal(barrier, inc=1, device_id={"mp": partner}, device_id_type=MESH)
    for offset in range(1, chips):
        pl.semaphore_signal(barrier, inc=1, device_id={"mp": peer(offset)}, device_id_type=MESH)
    for which in range(2):
        pl.semaphore_signal(barrier, inc=1, device_id={"dp": beside, "mp": 2 * chip + which}, device_id_type=MESH)
    greeted = chips + 2

    count_copy.wait()
    live_count = counts[me, data]
    mine, theirs = Load(counts, chip, data, positions), Load(counts, chip, beside, positions)

    for slot in range(group):
        x_copy(slot).wait()
        a_copy(slot).wait()
    for slot in range(group, slots):
        x_copy(slot).start()
        a_copy(slot).start()
    for owner in range(members):
        g_copy(owner).start()

    @pl.loop(0, slots // group)
    def _(turn):
        batch = [turn * group + at for at in range(group)]

        @pl.when(turn > 0)
        def _():
            for slot in batch:
                x_copy(slot).wait()
                a_copy(slot).wait()

        found = newton_roots([a_buf[slot] for slot in batch], [x_buf[slot] for slot in batch])
        for slot, root in zip(batch, found):
            live = jnp.full(root.shape, slot, jnp.int32) < live_count
            pool[core, slot] = jnp.where(live, root, 0.0).astype(jnp.bfloat16)

        @pl.when(turn == 0)
        def _():
            pl.semaphore_wait(barrier, greeted)
            for offset in range(1, chips):
                first_copy(offset).start()
            for number in range(relays):
                @pl.when(core == relayed_block(number)[0])
                def _():
                    for which in range(2):
                        relay_copy(number, which).start()

        for slot in batch:
            p_copy(core, slot).start()

    def launch(position, excess, taken=None):
        at_core, at_slot = packed_at(position + excess, mine.first, mine.second, slots)
        value = pool[at_core, at_slot, rows_of(core)]
        if taken is not None:
            value = lax.select_n(taken < theirs.excess, value, relayed[taken])
        staged[position - 2] = value
        for offset in range(1, chips):
            y_copy(offset, position).start()

    def near_apply(which):
        @pl.loop(0, slots // group)
        def _(turn):
            for at in range(group):
                slot = turn * group + at
                near[which, slot] = dot(pool[which, slot], g_buf[2 * chip + which, slot]).astype(near.dtype)

    for owner in range(members):
        g_copy(owner).wait()
    near_apply(core)

    @pl.loop(0, slots)
    def _(slot):
        p_copy(other, slot).wait_recv()

    @pl.loop(2, window)
    def _(position):
        launch(position, mine.excess)

    for number in range(relays):
        relay_copy(number, core).wait_recv()
        launch(window + number, mine.excess - theirs.excess, number)

    @pl.loop(window + relays, positions)
    def _(position):
        launch(position, mine.excess - theirs.excess)

    near_apply(other)
    last = far.shape[1] - 1
    for at in range(chips - 1):
        far[at, last] = jnp.zeros(far.shape[2:], far.dtype)

    loads = {offset: (Load(counts, source_of(offset), data, positions), Load(counts, source_of(offset), beside, positions))
             for offset in range(1, chips)}

    def arrive(kind, number):
        for offset in range(1, chips):
            if kind == "first":
                first_copy(offset).wait_recv()
                first_forward(offset, core).start()
            elif kind == "position":
                y_copy(offset, number).wait_recv()
                forward(offset, number, core).start()
                if window <= number < window + relays:
                    back_copy(offset, number - window).start()
            else:
                back_copy(offset, number).wait_recv()
                back_forward(offset, number, core).start()

    def apply(offset, kind, number):
        source = source_of(offset)
        at = offset - 1
        if kind == "first":
            first_forward(offset, other).wait_recv()
            for which in range(2):
                far[at, which] = dot(landed[at, which], g_buf[2 * source + which, 0]).astype(far.dtype)
        elif kind == "position":
            forward(offset, number, other).wait_recv()
            own, side = loads[offset]
            index = number + own.excess
            if number >= window:
                index = index - side.excess
            at_core, at_slot = packed_at(index, own.first, own.second, slots)
            far[at, number] = dot(landed[at, number], g_buf[2 * source + at_core, at_slot]).astype(far.dtype)
        else:
            back_forward(offset, number, other).wait_recv()
            at_core, at_slot = relayed_block(number)
            far[at, positions + number] = dot(returned[at, number], g_buf[2 * source + at_core, at_slot]).astype(far.dtype)

    events = [(2.0, "first", 0)]
    events += [(position + 1.0, "position", position) for position in range(2, positions)]
    events += [(window + number + 3.6, "back", number) for number in range(relays)]
    events = [event[1:] for event in sorted(events)]
    arrive(*events[0])
    for before, now in zip(events, events[1:]):
        arrive(*now)
        for offset in range(1, chips):
            apply(offset, *before)
    for offset in range(1, chips):
        apply(offset, *events[-1])

    @pl.loop(0, slots)
    def _(slot):
        p_copy(core, slot).wait_send()

    for number in range(relays):
        @pl.when(core == relayed_block(number)[0])
        def _():
            for which in range(2):
                relay_copy(number, which).wait_send()

    for offset in range(1, chips):
        first_copy(offset).wait_send()
        first_forward(offset, core).wait_send()
        for number in range(relays):
            back_copy(offset, number).wait_send()
            back_forward(offset, number, core).wait_send()

        @pl.loop(2, positions)
        def _(position):
            y_copy(offset, position).wait_send()
            forward(offset, position, core).wait_send()


def placing_kernel(members, positions, relays, window, count_table, near, far, out, counts, count_sem, near_sem, far_sem):
    me = lax.axis_index("mp")
    data = lax.axis_index("dp")
    chips = members // 2
    chip = me // 2
    slots = near.shape[1]
    count_copy = pltpu.make_async_copy(count_table, counts, count_sem)
    count_copy.start()

    def near_copy(which):
        return pltpu.make_async_copy(near.at[which], out.at[2 * chip + which], near_sem.at[which])

    for which in range(2):
        near_copy(which).start()
    count_copy.wait()
    copies = []
    for offset in range(1, chips):
        source = lax.rem(chip + chips - offset, chips)
        own, side = Load(counts, source, data, positions), Load(counts, source, neighbour_of(data), positions)
        both = jnp.minimum(own.first, own.second)
        for which in range(2):
            for slot in range(slots):
                index = jnp.where(slot < both, 2 * slot + which, slot + both)
                kept = jnp.where(index < 2, index, index - own.excess)
                place = jnp.where(kept < window, kept, kept + side.excess)
                handed = (index >= 2) & (index < 2 + own.excess)
                place = jnp.where(handed, positions + index - 2, place)
                place = jnp.where(slot < (own.first, own.second)[which], place, far.shape[1] - 1)
                copies.append(pltpu.make_async_copy(
                    far.at[offset - 1, place], out.at[2 * source + which, slot], far_sem.at[offset - 1, which, slot]))
                copies[-1].start()
    for which in range(2):
        near_copy(which).wait()
    for copy in copies:
        copy.wait()


def exchange(members, number, positions, relays, window, stats, prev_roots, counts, grads):
    slots, size = stats.shape[1], stats.shape[2]
    chips = members // 2
    square = (size, size)
    near = (2, slots) + square
    far = (chips - 1, positions + relays + 1) + square
    kept = grads.dtype.itemsize * size * size * (near[0] * near[1] + far[0] * far[1])
    semaphores = pltpu.SemaphoreType.DMA
    steps, backs = (chips - 1, positions - 1), (chips - 1, relays)
    near, far = pl.pallas_call(
        functools.partial(kernel, members, positions, relays, window),
        out_shape=(pltpu.VMEM(near, grads.dtype), pltpu.VMEM(far, grads.dtype)),
        in_specs=[pl.BlockSpec(memory_space=pltpu.HBM)] * 4,
        out_specs=(pl.BlockSpec(memory_space=pltpu.VMEM), pl.BlockSpec(memory_space=pltpu.VMEM)),
        scratch_shapes=[
            pltpu.SMEM(counts.shape, counts.dtype),
            semaphores,
            pltpu.VMEM((slots,) + square, jnp.float32),
            pltpu.VMEM((slots,) + square, jnp.float32),
            pltpu.VMEM(grads.shape, grads.dtype),
            pltpu.VMEM((2, slots) + square, jnp.bfloat16),
            pltpu.VMEM((positions - 2, size // 2, size), jnp.bfloat16),
            pltpu.VMEM((chips - 1, positions) + square, jnp.bfloat16),
            pltpu.VMEM((relays, size // 2, size), jnp.bfloat16),
            pltpu.VMEM((chips - 1, relays) + square, jnp.bfloat16),
            semaphores((slots,)),
            semaphores((slots,)),
            semaphores((members,)),
            semaphores(steps),
            semaphores(steps),
            semaphores((slots,)),
            semaphores((slots,)),
            semaphores(steps),
            semaphores(steps),
            semaphores((relays, 2)),
            semaphores((relays,)),
            semaphores(backs),
            semaphores(backs),
            semaphores(backs),
            semaphores(backs),
        ],
        compiler_params=pltpu.CompilerParams(
            collective_id=number, has_side_effects=True, vmem_limit_bytes=VMEM_BYTES - kept),
    )(counts, stats, prev_roots, grads)
    return pl.pallas_call(
        functools.partial(placing_kernel, members, positions, relays, window),
        out_shape=pltpu.HBM(grads.shape, grads.dtype),
        in_specs=[
            pl.BlockSpec(memory_space=pltpu.HBM),
            pl.BlockSpec(memory_space=pltpu.VMEM),
            pl.BlockSpec(memory_space=pltpu.VMEM),
        ],
        out_specs=pl.BlockSpec(memory_space=pltpu.HBM),
        scratch_shapes=[
            pltpu.SMEM(counts.shape, counts.dtype),
            semaphores,
            semaphores((2,)),
            semaphores((chips - 1, 2, slots)),
        ],
        compiler_params=pltpu.CompilerParams(vmem_limit_bytes=1 << 20),
    )(counts, near, far)


def local(members, stats, prev_roots, counts, grads):
    slots = stats.shape[1]
    sizes = list(range(slots + 1, slots + 5)) + [2 * slots]
    choice = pl.pallas_call(
        functools.partial(choosing_kernel, sizes, RELAYS),
        out_shape=jax.ShapeDtypeStruct((1,), jnp.int32),
        in_specs=[pl.BlockSpec(memory_space=pltpu.SMEM)],
        out_specs=pl.BlockSpec(memory_space=pltpu.SMEM),
    )(counts)
    branches = [functools.partial(exchange, members, number, size, RELAYS, WINDOW) for number, size in enumerate(sizes)]
    return lax.switch(choice[0], branches, stats, prev_roots, counts, grads)


def solution(mesh):
    return jax.shard_map(
        functools.partial(local, mesh.shape["mp"]),
        mesh=mesh,
        in_specs=(
            P("mp", "dp", None, None),
            P("mp", "dp", None, None),
            P(),
            P(None, "dp", None, "mp"),
        ),
        out_specs=P(None, "dp", None, "mp"),
        check_vma=False,
    )
```

```python
import functools

import jax
import jax.numpy as jnp
from jax import lax
from jax.experimental import pallas as pl
from jax.experimental.pallas import tpu as pltpu
from jax.sharding import PartitionSpec as P

VMEM_BYTES = 67043328 - 65536
MESH = pl.DeviceIdType.MESH
RELAYS = 3
WINDOW = 3
GROUP = 4


def dot(left, right):
    return jnp.dot(left.astype(jnp.bfloat16), right.astype(jnp.bfloat16), preferred_element_type=jnp.float32)


def shifted_squares(parts):
    return [2.0 * part + dot(part, part) for part in parts]


def newton_roots(statistics, initials):
    size = initials[0].shape[-1]
    rows = lax.broadcasted_iota(jnp.int32, (size, size), 0)
    columns = lax.broadcasted_iota(jnp.int32, (size, size), 1)
    identity = jnp.where(rows == columns, 1.0, 0.0).astype(jnp.float32)
    fourths = shifted_squares(shifted_squares([initial - identity for initial in initials]))
    moments = [statistic + dot(fourth, statistic) for fourth, statistic in zip(fourths, statistics)]
    changes = [0.25 * (identity - moment) for moment in moments]
    estimates = [initial + dot(initial, change) for initial, change in zip(initials, changes)]
    fourths = shifted_squares(shifted_squares(changes))
    moments = [moment + dot(fourth, moment) for fourth, moment in zip(fourths, moments)]
    changes = [0.25 * (identity - moment) for moment in moments]
    return [estimate + dot(estimate, change) for estimate, change in zip(estimates, changes)]


def packed_at(index, first, second, slots):
    both = jnp.minimum(first, second)
    paired = index < 2 * both
    slot = jnp.where(paired, lax.div(index, 2), index - both)
    core = jnp.where(paired, lax.rem(index, 2), jnp.where(first > second, 0, 1))
    return core, jnp.clip(slot, 0, slots - 1)


def neighbour_of(data):
    return data + 1 - 2 * lax.rem(data, 2)


def relayed_block(number):
    return number % 2, 1 + number // 2


class Load:
    def __init__(self, counts, chip, data, positions):
        self.first, self.second = counts[2 * chip, data], counts[2 * chip + 1, data]
        self.excess = jnp.maximum(self.first + self.second - positions, 0)


def opening_kernel(sizes, relays, count_table, stats, starts, choice, counts, first_a, first_x, count_sem, a_sem, x_sem):
    group = first_a.shape[0]
    copies = [pltpu.make_async_copy(count_table, counts, count_sem)]
    copies += [pltpu.make_async_copy(starts.at[0, slot], first_x.at[slot], x_sem.at[slot]) for slot in range(group)]
    copies += [pltpu.make_async_copy(stats.at[0, slot], first_a.at[slot], a_sem.at[slot]) for slot in range(group)]
    for copy in copies:
        copy.start()
    copies[0].wait()
    members, workers = counts.shape
    need = jnp.int32(0)
    for chip in range(members // 2):
        for data in range(0, workers, 2):
            pair = [counts[2 * chip, at] + counts[2 * chip + 1, at] for at in (data, data + 1)]
            need = jnp.maximum(need, lax.div(pair[0] + pair[1] + 1, 2))
            need = jnp.maximum(need, jnp.maximum(*pair) - relays)
    choice[0] = sum((need > size).astype(jnp.int32) for size in sizes[:-1])
    for copy in copies[1:]:
        copy.wait()


def kernel(members, positions, relays, window, counts, first_a, first_x, stats, starts, grads, near, far, a_buf, x_buf, g_buf, low, high, staged, landed, relayed, returned, a_sem, x_sem, g_sem, y_send, y_recv, p_send, p_recv,
           f_send, f_recv, r_send, r_recv, b_send, b_recv, h_send, h_recv):
    me = lax.axis_index("mp")
    data = lax.axis_index("dp")
    slots, size = stats.shape[1], stats.shape[2]
    chips = members // 2
    core = lax.rem(me, 2)
    chip = me // 2
    other = 1 - core
    partner = 2 * chip + other
    beside = neighbour_of(data)
    half = size // 2
    group = first_a.shape[0]

    def rows_of(which):
        return pl.ds(pl.multiple_of(which * half, half), half)

    def peer(offset):
        return lax.rem(chip + offset, chips) * 2 + core

    def source_of(offset):
        return lax.rem(chip + chips - offset, chips)

    def a_copy(slot):
        return pltpu.make_async_copy(stats.at[0, slot], a_buf.at[slot - group], a_sem.at[slot - group])

    def x_copy(slot):
        return pltpu.make_async_copy(starts.at[0, slot], x_buf.at[slot - group], x_sem.at[slot - group])

    def g_copy(owner):
        return pltpu.make_async_copy(grads.at[owner], g_buf.at[owner], g_sem.at[owner])

    def send(source, place, target, send_sem, recv_sem):
        return pltpu.make_async_remote_copy(
            src_ref=source, dst_ref=place, send_sem=send_sem, recv_sem=recv_sem,
            device_id=target, device_id_type=MESH)

    def p_copy(which, slot, early=False):
        block = low.at[which, slot] if early else high.at[which, slot - group]
        return send(block, block, {"mp": partner}, p_send.at[slot], p_recv.at[slot])

    def first_copy(offset):
        return send(low.at[core, 0], landed.at[offset - 1, core], {"mp": peer(offset)},
                    y_send.at[offset - 1, 0], y_recv.at[offset - 1, 0])

    def first_forward(offset, which):
        block = landed.at[offset - 1, which]
        return send(block, block, {"mp": partner}, f_send.at[offset - 1, 0], f_recv.at[offset - 1, 0])

    def y_copy(offset, position):
        return send(staged.at[position - 2], landed.at[offset - 1, position, rows_of(core)], {"mp": peer(offset)},
                    y_send.at[offset - 1, position - 1], y_recv.at[offset - 1, position - 1])

    def forward(offset, position, which):
        block = landed.at[offset - 1, position, rows_of(which)]
        return send(block, block, {"mp": partner}, f_send.at[offset - 1, position - 1], f_recv.at[offset - 1, position - 1])

    def relay_copy(number, which):
        at_core, at_slot = relayed_block(number)
        return send(low.at[at_core, at_slot, rows_of(which)], relayed.at[number], {"dp": beside, "mp": 2 * chip + which},
                    r_send.at[number, which], r_recv.at[number])

    def back_copy(offset, number):
        return send(landed.at[offset - 1, window + number, rows_of(core)], returned.at[offset - 1, number, rows_of(core)],
                    {"dp": beside, "mp": me}, b_send.at[offset - 1, number], b_recv.at[offset - 1, number])

    def back_forward(offset, number, which):
        block = returned.at[offset - 1, number, rows_of(which)]
        return send(block, block, {"mp": partner}, h_send.at[offset - 1, number], h_recv.at[offset - 1, number])

    barrier = pltpu.get_barrier_semaphore()
    pl.semaphore_signal(barrier, inc=1, device_id={"mp": partner}, device_id_type=MESH)
    for offset in range(1, chips):
        pl.semaphore_signal(barrier, inc=1, device_id={"mp": peer(offset)}, device_id_type=MESH)
    for which in range(2):
        pl.semaphore_signal(barrier, inc=1, device_id={"dp": beside, "mp": 2 * chip + which}, device_id_type=MESH)
    greeted = chips + 2
    for slot in range(group, slots):
        x_copy(slot).start()
        a_copy(slot).start()

    live_count = counts[me, data]
    mine, theirs = Load(counts, chip, data, positions), Load(counts, chip, beside, positions)

    def compute(batch, a_blocks, x_blocks):
        found = newton_roots(a_blocks, x_blocks)
        for slot, root in zip(batch, found):
            live = jnp.full(root.shape, slot, jnp.int32) < live_count
            yield slot, jnp.where(live, root, 0.0).astype(jnp.bfloat16)

    for slot, root in compute(range(group), [first_a[at] for at in range(group)], [first_x[at] for at in range(group)]):
        low[core, slot] = root
    pl.semaphore_wait(barrier, greeted)
    for offset in range(1, chips):
        first_copy(offset).start()
    for number in range(relays):
        @pl.when(core == relayed_block(number)[0])
        def _():
            for which in range(2):
                relay_copy(number, which).start()
    for slot in range(group):
        p_copy(core, slot, True).start()
    for owner in range(members):
        g_copy(owner).start()

    @pl.loop(1, slots // group)
    def _(turn):
        batch = [turn * group + at for at in range(group)]
        for slot in batch:
            x_copy(slot).wait()
            a_copy(slot).wait()
        for slot, root in compute(batch, [a_buf[slot - group] for slot in batch], [x_buf[slot - group] for slot in batch]):
            high[core, slot - group] = root
        for slot in batch:
            p_copy(core, slot).start()

    def launch(position, excess, early=False, taken=None):
        at_core, at_slot = packed_at(position + excess, mine.first, mine.second, slots)
        value = low[at_core, jnp.minimum(at_slot, group - 1), rows_of(core)]
        if not early:
            later = high[at_core, jnp.maximum(at_slot - group, 0), rows_of(core)]
            value = lax.select_n(at_slot >= group, value, later)
        if taken is not None:
            value = lax.select_n(taken < theirs.excess, value, relayed[taken])
        staged[position - 2] = value
        for offset in range(1, chips):
            y_copy(offset, position).start()

    def near_apply(which):
        for at in range(group):
            near[which, at] = dot(low[which, at], g_buf[2 * chip + which, at]).astype(near.dtype)

        @pl.loop(1, slots // group)
        def _(turn):
            for at in range(group):
                slot = turn * group + at
                near[which, slot] = dot(high[which, slot - group], g_buf[2 * chip + which, slot]).astype(near.dtype)

    def receive(early):
        @pl.loop(0 if early else group, group if early else slots)
        def _(slot):
            p_copy(other, slot, early).wait_recv()

    receive(True)
    for position in range(2, window):
        launch(position, mine.excess, True)
    for number in range(relays):
        position = window + number
        if position == group + 1:
            for owner in range(members):
                g_copy(owner).wait()
            near_apply(core)
            receive(False)
        relay_copy(number, core).wait_recv()
        launch(position, mine.excess - theirs.excess, position <= group, number)

    @pl.loop(window + relays, positions)
    def _(position):
        launch(position, mine.excess - theirs.excess)

    near_apply(other)
    last = far.shape[1] - 1
    for at in range(chips - 1):
        far[at, last] = jnp.zeros(far.shape[2:], far.dtype)

    loads = {offset: (Load(counts, source_of(offset), data, positions), Load(counts, source_of(offset), beside, positions))
             for offset in range(1, chips)}

    def arrive(kind, number):
        for offset in range(1, chips):
            if kind == "first":
                first_copy(offset).wait_recv()
                first_forward(offset, core).start()
            elif kind == "position":
                y_copy(offset, number).wait_recv()
                forward(offset, number, core).start()
                if window <= number < window + relays:
                    back_copy(offset, number - window).start()
            else:
                back_copy(offset, number).wait_recv()
                back_forward(offset, number, core).start()

    def apply(offset, kind, number):
        source = source_of(offset)
        at = offset - 1
        if kind == "first":
            first_forward(offset, other).wait_recv()
            for which in range(2):
                far[at, which] = dot(landed[at, which], g_buf[2 * source + which, 0]).astype(far.dtype)
        elif kind == "position":
            forward(offset, number, other).wait_recv()
            own, side = loads[offset]
            index = number + own.excess
            if number >= window:
                index = index - side.excess
            at_core, at_slot = packed_at(index, own.first, own.second, slots)
            far[at, number] = dot(landed[at, number], g_buf[2 * source + at_core, at_slot]).astype(far.dtype)
        else:
            back_forward(offset, number, other).wait_recv()
            at_core, at_slot = relayed_block(number)
            far[at, positions + number] = dot(returned[at, number], g_buf[2 * source + at_core, at_slot]).astype(far.dtype)

    events = [(2.0, "first", 0)]
    events += [(position + 1.0, "position", position) for position in range(2, positions)]
    events += [(window + number + 3.6, "back", number) for number in range(relays)]
    events = [event[1:] for event in sorted(events)]
    arrive(*events[0])
    for before, now in zip(events, events[1:]):
        arrive(*now)
        for offset in range(1, chips):
            apply(offset, *before)
    for offset in range(1, chips):
        apply(offset, *events[-1])

    @pl.loop(0, group)
    def _(slot):
        p_copy(core, slot, True).wait_send()

    @pl.loop(group, slots)
    def _(slot):
        p_copy(core, slot).wait_send()

    for number in range(relays):
        @pl.when(core == relayed_block(number)[0])
        def _():
            for which in range(2):
                relay_copy(number, which).wait_send()

    for offset in range(1, chips):
        first_copy(offset).wait_send()
        first_forward(offset, core).wait_send()
        for number in range(relays):
            back_copy(offset, number).wait_send()
            back_forward(offset, number, core).wait_send()

        @pl.loop(2, positions)
        def _(position):
            y_copy(offset, position).wait_send()
            forward(offset, position, core).wait_send()


def placing_kernel(members, positions, relays, window, counts, near, far, out, near_sem, far_sem):
    me = lax.axis_index("mp")
    data = lax.axis_index("dp")
    chips = members // 2
    chip = me // 2
    slots = near.shape[1]

    def near_copy(which):
        return pltpu.make_async_copy(near.at[which], out.at[2 * chip + which], near_sem.at[which])

    for which in range(2):
        near_copy(which).start()
    copies = []
    for offset in range(1, chips):
        source = lax.rem(chip + chips - offset, chips)
        own, side = Load(counts, source, data, positions), Load(counts, source, neighbour_of(data), positions)
        both = jnp.minimum(own.first, own.second)
        for which in range(2):
            for slot in range(slots):
                index = jnp.where(slot < both, 2 * slot + which, slot + both)
                kept = jnp.where(index < 2, index, index - own.excess)
                place = jnp.where(kept < window, kept, kept + side.excess)
                handed = (index >= 2) & (index < 2 + own.excess)
                place = jnp.where(handed, positions + index - 2, place)
                place = jnp.where(slot < (own.first, own.second)[which], place, far.shape[1] - 1)
                copies.append(pltpu.make_async_copy(
                    far.at[offset - 1, place], out.at[2 * source + which, slot], far_sem.at[offset - 1, which, slot]))
                copies[-1].start()
    for which in range(2):
        near_copy(which).wait()
    for copy in copies:
        copy.wait()


def exchange(members, number, positions, relays, window, counts, first_a, first_x, stats, prev_roots, grads):
    slots, size = stats.shape[1], stats.shape[2]
    chips = members // 2
    square = (size, size)
    near = (2, slots) + square
    far = (chips - 1, positions + relays + 1) + square
    group = first_a.shape[0]
    kept = grads.dtype.itemsize * size * size * (near[0] * near[1] + far[0] * far[1])
    kept += 2 * first_a.size * first_a.dtype.itemsize
    semaphores = pltpu.SemaphoreType.DMA
    steps, backs = (chips - 1, positions - 1), (chips - 1, relays)
    near, far = pl.pallas_call(
        functools.partial(kernel, members, positions, relays, window),
        out_shape=(pltpu.VMEM(near, grads.dtype), pltpu.VMEM(far, grads.dtype)),
        in_specs=[pl.BlockSpec(memory_space=space)
                  for space in (pltpu.SMEM, pltpu.VMEM, pltpu.VMEM, pltpu.HBM, pltpu.HBM, pltpu.HBM)],
        out_specs=(pl.BlockSpec(memory_space=pltpu.VMEM), pl.BlockSpec(memory_space=pltpu.VMEM)),
        scratch_shapes=[
            pltpu.VMEM((slots - group,) + square, jnp.float32),
            pltpu.VMEM((slots - group,) + square, jnp.float32),
            pltpu.VMEM(grads.shape, grads.dtype),
            pltpu.VMEM((2, group) + square, jnp.bfloat16),
            pltpu.VMEM((2, slots - group) + square, jnp.bfloat16),
            pltpu.VMEM((positions - 2, size // 2, size), jnp.bfloat16),
            pltpu.VMEM((chips - 1, positions) + square, jnp.bfloat16),
            pltpu.VMEM((relays, size // 2, size), jnp.bfloat16),
            pltpu.VMEM((chips - 1, relays) + square, jnp.bfloat16),
            semaphores((slots - group,)),
            semaphores((slots - group,)),
            semaphores((members,)),
            semaphores(steps),
            semaphores(steps),
            semaphores((slots,)),
            semaphores((slots,)),
            semaphores(steps),
            semaphores(steps),
            semaphores((relays, 2)),
            semaphores((relays,)),
            semaphores(backs),
            semaphores(backs),
            semaphores(backs),
            semaphores(backs),
        ],
        compiler_params=pltpu.CompilerParams(
            collective_id=number, has_side_effects=True, vmem_limit_bytes=VMEM_BYTES - kept),
    )(counts, first_a, first_x, stats, prev_roots, grads)
    return pl.pallas_call(
        functools.partial(placing_kernel, members, positions, relays, window),
        out_shape=pltpu.HBM(grads.shape, grads.dtype),
        in_specs=[
            pl.BlockSpec(memory_space=pltpu.SMEM),
            pl.BlockSpec(memory_space=pltpu.VMEM),
            pl.BlockSpec(memory_space=pltpu.VMEM),
        ],
        out_specs=pl.BlockSpec(memory_space=pltpu.HBM),
        scratch_shapes=[
            semaphores((2,)),
            semaphores((chips - 1, 2, slots)),
        ],
        compiler_params=pltpu.CompilerParams(vmem_limit_bytes=1 << 20),
    )(counts, near, far)


def local(members, stats, prev_roots, counts, grads):
    slots = stats.shape[1]
    sizes = list(range(slots + 1, slots + 5)) + [2 * slots]
    first = (GROUP,) + stats.shape[2:]
    semaphores = pltpu.SemaphoreType.DMA
    choice, table, first_a, first_x = pl.pallas_call(
        functools.partial(opening_kernel, sizes, RELAYS),
        out_shape=(pltpu.SMEM((1,), jnp.int32), pltpu.SMEM(counts.shape, counts.dtype),
                   pltpu.VMEM(first, stats.dtype), pltpu.VMEM(first, stats.dtype)),
        in_specs=[pl.BlockSpec(memory_space=pltpu.HBM)] * 3,
        out_specs=tuple(pl.BlockSpec(memory_space=space) for space in (pltpu.SMEM, pltpu.SMEM, pltpu.VMEM, pltpu.VMEM)),
        scratch_shapes=[semaphores, semaphores((GROUP,)), semaphores((GROUP,))],
        compiler_params=pltpu.CompilerParams(vmem_limit_bytes=1 << 20),
    )(pltpu.with_memory_space_constraint(counts, pltpu.HBM), stats, prev_roots)
    branches = [functools.partial(exchange, members, number, size, RELAYS, WINDOW) for number, size in enumerate(sizes)]
    return lax.switch(choice[0], branches, table, first_a, first_x, stats, prev_roots, grads)


def solution(mesh):
    return jax.shard_map(
        functools.partial(local, mesh.shape["mp"]),
        mesh=mesh,
        in_specs=(
            P("mp", "dp", None, None),
            P("mp", "dp", None, None),
            P(),
            P(None, "dp", None, "mp"),
        ),
        out_specs=P(None, "dp", None, "mp"),
        check_vma=False,
    )
```

```python
import functools

import jax
import jax.numpy as jnp
from jax import lax
from jax.experimental import pallas as pl
from jax.experimental.pallas import tpu as pltpu
from jax.sharding import PartitionSpec as P

VMEM_BYTES = 67043328 - 65536
MESH = pl.DeviceIdType.MESH
RELAYS = 3
WINDOW = 3
BACK = 3.6
GROUP = 4


def dot(left, right):
    return jnp.dot(left.astype(jnp.bfloat16), right.astype(jnp.bfloat16), preferred_element_type=jnp.float32)


def shifted_squares(parts):
    return [2.0 * part + dot(part, part) for part in parts]


def newton_roots(statistics, initials):
    size = initials[0].shape[-1]
    rows = lax.broadcasted_iota(jnp.int32, (size, size), 0)
    columns = lax.broadcasted_iota(jnp.int32, (size, size), 1)
    identity = jnp.where(rows == columns, 1.0, 0.0).astype(jnp.float32)
    fourths = shifted_squares(shifted_squares([initial - identity for initial in initials]))
    moments = [statistic + dot(fourth, statistic) for fourth, statistic in zip(fourths, statistics)]
    changes = [0.25 * (identity - moment) for moment in moments]
    estimates = [initial + dot(initial, change) for initial, change in zip(initials, changes)]
    fourths = shifted_squares(shifted_squares(changes))
    moments = [moment + dot(fourth, moment) for fourth, moment in zip(fourths, moments)]
    changes = [0.25 * (identity - moment) for moment in moments]
    return [estimate + dot(estimate, change) for estimate, change in zip(estimates, changes)]


def packed_at(index, first, second, slots):
    both = jnp.minimum(first, second)
    paired = index < 2 * both
    slot = jnp.where(paired, lax.div(index, 2), index - both)
    core = jnp.where(paired, lax.rem(index, 2), jnp.where(first > second, 0, 1))
    return core, jnp.clip(slot, 0, slots - 1)


def neighbour_of(data):
    return data + 1 - 2 * lax.rem(data, 2)


def relayed_block(number):
    return 0, 1 + number


def kept_index(number, excess):
    number = jnp.maximum(number, 2)
    return jnp.minimum(2 * number - 1, number + excess)


def capacity(positions, spared, data):
    return positions - spared * (data == 0).astype(jnp.int32)


class Load:
    def __init__(self, counts, chip, data, positions, spared):
        self.first, self.second = counts[2 * chip, data], counts[2 * chip + 1, data]
        self.excess = jnp.maximum(self.first + self.second - capacity(positions, spared, data), 0)


def opening_kernel(sizes, relays, count_table, stats, starts, choice, counts, first_a, first_x, count_sem, a_sem, x_sem):
    group = first_a.shape[0]
    copies = [pltpu.make_async_copy(count_table, counts, count_sem)]
    copies += [pltpu.make_async_copy(starts.at[0, slot], first_x.at[slot], x_sem.at[slot]) for slot in range(group)]
    copies += [pltpu.make_async_copy(stats.at[0, slot], first_a.at[slot], a_sem.at[slot]) for slot in range(group)]
    for copy in copies:
        copy.start()
    copies[0].wait()
    members, workers = counts.shape
    need = jnp.int32(0)
    for chip in range(members // 2):
        for data in range(0, workers, 2):
            pair = [counts[2 * chip, at] + counts[2 * chip + 1, at] for at in (data, data + 1)]
            spared = int(data == 0)
            least = lax.div(pair[0] + pair[1] + 1 + spared, 2)
            least = jnp.maximum(least, jnp.maximum(pair[0] + spared, pair[1]) - relays)
            if spared:
                both = jnp.minimum(counts[2 * chip, data], counts[2 * chip + 1, data])
                over = pair[0] - (sizes[0] - 1)
                least = jnp.where((over > 0) & (both <= over), jnp.maximum(least, sizes[1]), least)
            need = jnp.maximum(need, least)
    choice[0] = sum((need > size).astype(jnp.int32) for size in sizes[:-1])
    for copy in copies[1:]:
        copy.wait()


def kernel(members, positions, spared, relays, window, counts, first_a, first_x, stats, starts, grads, near, far, a_buf, x_buf, g_buf, low, high, staged, landed, relayed, returned, a_sem, x_sem, g_sem, y_send, y_recv, p_send, p_recv,
           f_send, f_recv, r_send, r_recv, b_send, b_recv, h_send, h_recv):
    me = lax.axis_index("mp")
    data = lax.axis_index("dp")
    slots, size = stats.shape[1], stats.shape[2]
    chips = members // 2
    core = lax.rem(me, 2)
    chip = me // 2
    other = 1 - core
    partner = 2 * chip + other
    beside = neighbour_of(data)
    half = size // 2
    group = first_a.shape[0]

    def rows_of(which):
        return pl.ds(pl.multiple_of(which * half, half), half)

    def peer(offset):
        return lax.rem(chip + offset, chips) * 2 + core

    def source_of(offset):
        return lax.rem(chip + chips - offset, chips)

    def a_copy(slot):
        return pltpu.make_async_copy(stats.at[0, slot], a_buf.at[slot - group], a_sem.at[slot - group])

    def x_copy(slot):
        return pltpu.make_async_copy(starts.at[0, slot], x_buf.at[slot - group], x_sem.at[slot - group])

    def g_copy(owner):
        return pltpu.make_async_copy(grads.at[owner], g_buf.at[owner], g_sem.at[owner])

    def send(source, place, target, send_sem, recv_sem):
        return pltpu.make_async_remote_copy(
            src_ref=source, dst_ref=place, send_sem=send_sem, recv_sem=recv_sem,
            device_id=target, device_id_type=MESH)

    def p_copy(which, slot, early=False):
        block = low.at[which, slot] if early else high.at[which, slot - group]
        return send(block, block, {"mp": partner}, p_send.at[slot], p_recv.at[slot])

    def first_copy(offset):
        return send(low.at[core, 0], landed.at[offset - 1, core], {"mp": peer(offset)},
                    y_send.at[offset - 1, 0], y_recv.at[offset - 1, 0])

    def first_forward(offset, which):
        block = landed.at[offset - 1, which]
        return send(block, block, {"mp": partner}, f_send.at[offset - 1, 0], f_recv.at[offset - 1, 0])

    def y_copy(offset, position):
        return send(staged.at[position - 2], landed.at[offset - 1, position, rows_of(core)], {"mp": peer(offset)},
                    y_send.at[offset - 1, position - 1], y_recv.at[offset - 1, position - 1])

    def forward(offset, position, which):
        block = landed.at[offset - 1, position, rows_of(which)]
        return send(block, block, {"mp": partner}, f_send.at[offset - 1, position - 1], f_recv.at[offset - 1, position - 1])

    def relay_copy(number, which):
        at_core, at_slot = relayed_block(number)
        return send(low.at[at_core, at_slot, rows_of(which)], relayed.at[number], {"dp": beside, "mp": 2 * chip + which},
                    r_send.at[number, which], r_recv.at[number])

    def back_copy(offset, number):
        return send(landed.at[offset - 1, window + number, rows_of(core)], returned.at[offset - 1, number, rows_of(core)],
                    {"dp": beside, "mp": me}, b_send.at[offset - 1, number], b_recv.at[offset - 1, number])

    def back_forward(offset, number, which):
        block = returned.at[offset - 1, number, rows_of(which)]
        return send(block, block, {"mp": partner}, h_send.at[offset - 1, number], h_recv.at[offset - 1, number])

    barrier = pltpu.get_barrier_semaphore()
    pl.semaphore_signal(barrier, inc=1, device_id={"mp": partner}, device_id_type=MESH)
    for offset in range(1, chips):
        pl.semaphore_signal(barrier, inc=1, device_id={"mp": peer(offset)}, device_id_type=MESH)
    for which in range(2):
        pl.semaphore_signal(barrier, inc=1, device_id={"dp": beside, "mp": 2 * chip + which}, device_id_type=MESH)
    greeted = chips + 2
    for slot in range(group, slots):
        x_copy(slot).start()
        a_copy(slot).start()

    live_count = counts[me, data]
    mine, theirs = Load(counts, chip, data, positions, spared), Load(counts, chip, beside, positions, spared)

    def compute(batch, a_blocks, x_blocks):
        found = newton_roots(a_blocks, x_blocks)
        for slot, root in zip(batch, found):
            live = jnp.full(root.shape, slot, jnp.int32) < live_count
            yield slot, jnp.where(live, root, 0.0).astype(jnp.bfloat16)

    for slot, root in compute(range(group), [first_a[at] for at in range(group)], [first_x[at] for at in range(group)]):
        low[core, slot] = root
    pl.semaphore_wait(barrier, greeted)
    for offset in range(1, chips):
        first_copy(offset).start()
    for number in range(relays):
        @pl.when(core == relayed_block(number)[0])
        def _():
            for which in range(2):
                relay_copy(number, which).start()
    for slot in range(group):
        p_copy(core, slot, True).start()
    for owner in range(members):
        g_copy(owner).start()

    @pl.loop(1, slots // group)
    def _(turn):
        batch = [turn * group + at for at in range(group)]
        for slot in batch:
            x_copy(slot).wait()
            a_copy(slot).wait()
        for slot, root in compute(batch, [a_buf[slot - group] for slot in batch], [x_buf[slot - group] for slot in batch]):
            high[core, slot - group] = root
        for slot in batch:
            p_copy(core, slot).start()

    def launch(position, filled, early=False, taken=None):
        at_core, at_slot = packed_at(kept_index(position - filled, mine.excess), mine.first, mine.second, slots)
        value = low[at_core, jnp.minimum(at_slot, group - 1), rows_of(core)]
        if not early:
            later = high[at_core, jnp.maximum(at_slot - group, 0), rows_of(core)]
            value = lax.select_n(at_slot >= group, value, later)
        if taken is not None:
            value = lax.select_n(taken < theirs.excess, value, relayed[taken])
        staged[position - 2] = value
        for offset in range(1, chips):
            y_copy(offset, position).start()

    def near_apply(which):
        for at in range(group):
            near[which, at] = dot(low[which, at], g_buf[2 * chip + which, at]).astype(near.dtype)

        @pl.loop(1, slots // group)
        def _(turn):
            for at in range(group):
                slot = turn * group + at
                near[which, slot] = dot(high[which, slot - group], g_buf[2 * chip + which, slot]).astype(near.dtype)

    def receive(early):
        @pl.loop(0 if early else group, group if early else slots)
        def _(slot):
            p_copy(other, slot, early).wait_recv()

    receive(True)
    for position in range(2, window):
        launch(position, 0, True)
    for number in range(relays):
        position = window + number
        if position == group + 1:
            for owner in range(members):
                g_copy(owner).wait()
            near_apply(core)
            receive(False)
        relay_copy(number, core).wait_recv()
        launch(position, theirs.excess, position <= group, number)

    @pl.loop(window + relays, capacity(positions, spared, data))
    def _(position):
        launch(position, theirs.excess)

    near_apply(other)
    last = far.shape[1] - 1
    for at in range(chips - 1):
        far[at, last] = jnp.zeros(far.shape[2:], far.dtype)

    loads = {offset: [Load(counts, source_of(offset), at, positions, spared) for at in (data, beside)]
             for offset in range(1, chips)}

    def arrive(kind, number):
        for offset in range(1, chips):
            if kind == "first":
                first_copy(offset).wait_recv()
                first_forward(offset, core).start()
            elif kind == "position":
                y_copy(offset, number).wait_recv()
                forward(offset, number, core).start()
                if window <= number < window + relays:
                    back_copy(offset, number - window).start()
            else:
                back_copy(offset, number).wait_recv()
                back_forward(offset, number, core).start()

    def apply(offset, kind, number):
        source = source_of(offset)
        at = offset - 1
        if kind == "first":
            first_forward(offset, other).wait_recv()
            for which in range(2):
                far[at, which] = dot(landed[at, which], g_buf[2 * source + which, 0]).astype(far.dtype)
        elif kind == "position":
            forward(offset, number, other).wait_recv()
            own, side = loads[offset]
            index = kept_index(number - side.excess if number >= window else number, own.excess)
            at_core, at_slot = packed_at(index, own.first, own.second, slots)
            far[at, number] = dot(landed[at, number], g_buf[2 * source + at_core, at_slot]).astype(far.dtype)
        else:
            back_forward(offset, number, other).wait_recv()
            at_core, at_slot = relayed_block(number)
            far[at, positions + number] = dot(returned[at, number], g_buf[2 * source + at_core, at_slot]).astype(far.dtype)

    events = [(2.0, "first", 0)]
    events += [(position + 1.0, "position", position) for position in range(2, positions)]
    events += [(window + number + BACK, "back", number) for number in range(relays)]
    events = [event[1:] for event in sorted(events)]
    last_here = jnp.logical_or(spared == 0, data > 0)
    arrive(*events[0])
    for before, now in zip(events, events[1:]):
        if now == events[-1]:
            pl.when(last_here)(functools.partial(arrive, *now))
        else:
            arrive(*now)
        for offset in range(1, chips):
            apply(offset, *before)

    @pl.loop(0, group)
    def _(slot):
        p_copy(core, slot, True).wait_send()

    @pl.loop(group, slots)
    def _(slot):
        p_copy(core, slot).wait_send()

    for number in range(relays):
        @pl.when(core == relayed_block(number)[0])
        def _():
            for which in range(2):
                relay_copy(number, which).wait_send()

    def sent(offset, kind, number):
        if kind == "first":
            first_copy(offset).wait_send()
            first_forward(offset, core).wait_send()
        elif kind == "position":
            y_copy(offset, number).wait_send()
            forward(offset, number, core).wait_send()
        else:
            back_copy(offset, number).wait_send()
            back_forward(offset, number, core).wait_send()

    for event in events[:-1]:
        for offset in range(1, chips):
            sent(offset, *event)

    @pl.when(last_here)
    def _():
        for offset in range(1, chips):
            apply(offset, *events[-1])
            sent(offset, *events[-1])


def placing_kernel(members, positions, spared, relays, window, counts, near, far, out, near_sem, far_sem):
    me = lax.axis_index("mp")
    data = lax.axis_index("dp")
    chips = members // 2
    chip = me // 2
    slots = near.shape[1]

    def near_copy(which):
        return pltpu.make_async_copy(near.at[which], out.at[2 * chip + which], near_sem.at[which])

    for which in range(2):
        near_copy(which).start()
    copies = []
    for offset in range(1, chips):
        source = lax.rem(chip + chips - offset, chips)
        own, side = (Load(counts, source, at, positions, spared) for at in (data, neighbour_of(data)))
        both = jnp.minimum(own.first, own.second)
        for which in range(2):
            for slot in range(slots):
                index = jnp.where(slot < both, 2 * slot + which, slot + both)
                odd = lax.rem(index, 2)
                near_start = index <= 2 * own.excess + 1
                kept = jnp.where(index < 2, index, jnp.where(near_start, lax.div(index + 1, 2), index - own.excess))
                place = jnp.where(kept < window, kept, kept + side.excess)
                passed = (index >= 2) & near_start & (odd == 0)
                place = jnp.where(passed, positions + lax.div(index, 2) - 1, place)
                place = jnp.where(slot < (own.first, own.second)[which], place, far.shape[1] - 1)
                copies.append(pltpu.make_async_copy(
                    far.at[offset - 1, place], out.at[2 * source + which, slot], far_sem.at[offset - 1, which, slot]))
                copies[-1].start()
    for which in range(2):
        near_copy(which).wait()
    for copy in copies:
        copy.wait()


def exchange(members, number, positions, spared, relays, window, counts, first_a, first_x, stats, prev_roots, grads):
    slots, size = stats.shape[1], stats.shape[2]
    chips = members // 2
    square = (size, size)
    near = (2, slots) + square
    far = (chips - 1, positions + relays + 1) + square
    group = first_a.shape[0]
    kept = grads.dtype.itemsize * size * size * (near[0] * near[1] + far[0] * far[1])
    kept += 2 * first_a.size * first_a.dtype.itemsize
    semaphores = pltpu.SemaphoreType.DMA
    steps, backs = (chips - 1, positions - 1), (chips - 1, relays)
    near, far = pl.pallas_call(
        functools.partial(kernel, members, positions, spared, relays, window),
        out_shape=(pltpu.VMEM(near, grads.dtype), pltpu.VMEM(far, grads.dtype)),
        in_specs=[pl.BlockSpec(memory_space=space)
                  for space in (pltpu.SMEM, pltpu.VMEM, pltpu.VMEM, pltpu.HBM, pltpu.HBM, pltpu.HBM)],
        out_specs=(pl.BlockSpec(memory_space=pltpu.VMEM), pl.BlockSpec(memory_space=pltpu.VMEM)),
        scratch_shapes=[
            pltpu.VMEM((slots - group,) + square, jnp.float32),
            pltpu.VMEM((slots - group,) + square, jnp.float32),
            pltpu.VMEM(grads.shape, grads.dtype),
            pltpu.VMEM((2, group) + square, jnp.bfloat16),
            pltpu.VMEM((2, slots - group) + square, jnp.bfloat16),
            pltpu.VMEM((positions - 2, size // 2, size), jnp.bfloat16),
            pltpu.VMEM((chips - 1, positions) + square, jnp.bfloat16),
            pltpu.VMEM((relays, size // 2, size), jnp.bfloat16),
            pltpu.VMEM((chips - 1, relays) + square, jnp.bfloat16),
            semaphores((slots - group,)),
            semaphores((slots - group,)),
            semaphores((members,)),
            semaphores(steps),
            semaphores(steps),
            semaphores((slots,)),
            semaphores((slots,)),
            semaphores(steps),
            semaphores(steps),
            semaphores((relays, 2)),
            semaphores((relays,)),
            semaphores(backs),
            semaphores(backs),
            semaphores(backs),
            semaphores(backs),
        ],
        compiler_params=pltpu.CompilerParams(
            collective_id=number, has_side_effects=True, vmem_limit_bytes=VMEM_BYTES - kept),
    )(counts, first_a, first_x, stats, prev_roots, grads)
    return pl.pallas_call(
        functools.partial(placing_kernel, members, positions, spared, relays, window),
        out_shape=pltpu.HBM(grads.shape, grads.dtype),
        in_specs=[
            pl.BlockSpec(memory_space=pltpu.SMEM),
            pl.BlockSpec(memory_space=pltpu.VMEM),
            pl.BlockSpec(memory_space=pltpu.VMEM),
        ],
        out_specs=pl.BlockSpec(memory_space=pltpu.HBM),
        scratch_shapes=[
            semaphores((2,)),
            semaphores((chips - 1, 2, slots)),
        ],
        compiler_params=pltpu.CompilerParams(vmem_limit_bytes=1 << 20),
    )(counts, near, far)


def local(members, stats, prev_roots, counts, grads):
    slots = stats.shape[1]
    sizes = list(range(slots + 1, slots + 5)) + [2 * slots]
    first = (GROUP,) + stats.shape[2:]
    semaphores = pltpu.SemaphoreType.DMA
    choice, table, first_a, first_x = pl.pallas_call(
        functools.partial(opening_kernel, sizes, RELAYS),
        out_shape=(pltpu.SMEM((1,), jnp.int32), pltpu.SMEM(counts.shape, counts.dtype),
                   pltpu.VMEM(first, stats.dtype), pltpu.VMEM(first, stats.dtype)),
        in_specs=[pl.BlockSpec(memory_space=pltpu.HBM)] * 3,
        out_specs=tuple(pl.BlockSpec(memory_space=space) for space in (pltpu.SMEM, pltpu.SMEM, pltpu.VMEM, pltpu.VMEM)),
        scratch_shapes=[semaphores, semaphores((GROUP,)), semaphores((GROUP,))],
        compiler_params=pltpu.CompilerParams(vmem_limit_bytes=1 << 20),
    )(pltpu.with_memory_space_constraint(counts, pltpu.HBM), stats, prev_roots)
    branches = [functools.partial(exchange, members, number, size, int(size != sizes[-1]), RELAYS, WINDOW)
                for number, size in enumerate(sizes)]
    return lax.switch(choice[0], branches, table, first_a, first_x, stats, prev_roots, grads)


def solution(mesh):
    return jax.shard_map(
        functools.partial(local, mesh.shape["mp"]),
        mesh=mesh,
        in_specs=(
            P("mp", "dp", None, None),
            P("mp", "dp", None, None),
            P(),
            P(None, "dp", None, "mp"),
        ),
        out_specs=P(None, "dp", None, "mp"),
        check_vma=False,
    )
```

```python
import functools

import jax
import jax.numpy as jnp
from jax import lax
from jax.experimental import pallas as pl
from jax.experimental.pallas import tpu as pltpu
from jax.sharding import PartitionSpec as P

VMEM_BYTES = 67043328 - 65536
MESH = pl.DeviceIdType.MESH
RELAYS = 3
WINDOW = 3
BACK = 3.6
GROUP = 4


def dot(left, right):
    return jnp.dot(left.astype(jnp.bfloat16), right.astype(jnp.bfloat16), preferred_element_type=jnp.float32)


def shifted_squares(parts):
    return [2.0 * part + dot(part, part) for part in parts]


def newton_roots(statistics, initials):
    size = initials[0].shape[-1]
    rows = lax.broadcasted_iota(jnp.int32, (size, size), 0)
    columns = lax.broadcasted_iota(jnp.int32, (size, size), 1)
    identity = jnp.where(rows == columns, 1.0, 0.0).astype(jnp.float32)
    fourths = shifted_squares(shifted_squares([initial - identity for initial in initials]))
    moments = [statistic + dot(fourth, statistic) for fourth, statistic in zip(fourths, statistics)]
    changes = [0.25 * (identity - moment) for moment in moments]
    estimates = [initial + dot(initial, change) for initial, change in zip(initials, changes)]
    fourths = shifted_squares(shifted_squares(changes))
    moments = [moment + dot(fourth, moment) for fourth, moment in zip(fourths, moments)]
    changes = [0.25 * (identity - moment) for moment in moments]
    return [estimate + dot(estimate, change) for estimate, change in zip(estimates, changes)]


def packed_at(index, first, second, slots):
    both = jnp.minimum(first, second)
    paired = index < 2 * both
    slot = jnp.where(paired, lax.div(index, 2), index - both)
    core = jnp.where(paired, lax.rem(index, 2), jnp.where(first > second, 0, 1))
    return core, jnp.clip(slot, 0, slots - 1)


def neighbour_of(data):
    return data + 1 - 2 * lax.rem(data, 2)


def relayed_block(number):
    return 0, 1 + number


def kept_index(number, excess):
    number = jnp.maximum(number, 2)
    return jnp.minimum(2 * number - 1, number + excess)


def capacity(positions, spared, chip, data):
    return positions - spared * ((chip > 0).astype(jnp.int32) + (data == 0).astype(jnp.int32))


class Load:
    def __init__(self, counts, chip, data, positions, spared):
        self.first, self.second = counts[2 * chip, data], counts[2 * chip + 1, data]
        self.excess = jnp.maximum(self.first + self.second - capacity(positions, spared, chip, data), 0)


def opening_kernel(sizes, relays, slots, count_table, stats, starts, choice, counts, first_a, first_x, count_sem, a_sem, x_sem):
    group = first_a.shape[0]
    copies = [pltpu.make_async_copy(count_table, counts, count_sem)]
    copies += [pltpu.make_async_copy(starts.at[0, slot], first_x.at[slot], x_sem.at[slot]) for slot in range(group)]
    copies += [pltpu.make_async_copy(stats.at[0, slot], first_a.at[slot], a_sem.at[slot]) for slot in range(group)]
    for copy in copies:
        copy.start()
    copies[0].wait()
    members, workers = counts.shape
    need = jnp.int32(0)
    for chip in range(members // 2):
        for data in range(0, workers, 2):
            pair = [counts[2 * chip, at] + counts[2 * chip + 1, at] for at in (data, data + 1)]
            fewer = int(chip > 0)
            spared = int(data == 0)
            least = lax.div(pair[0] + pair[1] + 1 + spared, 2) + fewer
            least = jnp.maximum(least, jnp.maximum(pair[0] + spared, pair[1]) + fewer - relays)
            if sizes[0] - fewer - spared <= slots:
                both = jnp.minimum(counts[2 * chip, data], counts[2 * chip + 1, data])
                over = pair[0] - (sizes[0] - fewer - spared)
                least = jnp.where((over > 0) & (both <= over), jnp.maximum(least, sizes[1]), least)
            need = jnp.maximum(need, least)
    choice[0] = sum((need > size).astype(jnp.int32) for size in sizes[:-1])
    for copy in copies[1:]:
        copy.wait()


def kernel(members, positions, spared, relays, window, counts, first_a, first_x, stats, starts, grads, near, far, a_buf, x_buf, g_buf, low, high, staged, landed, relayed, returned, a_sem, x_sem, g_sem, y_send, y_recv, p_send, p_recv,
           f_send, f_recv, r_send, r_recv, b_send, b_recv, h_send, h_recv):
    me = lax.axis_index("mp")
    data = lax.axis_index("dp")
    slots, size = stats.shape[1], stats.shape[2]
    chips = members // 2
    core = lax.rem(me, 2)
    chip = me // 2
    other = 1 - core
    partner = 2 * chip + other
    beside = neighbour_of(data)
    half = size // 2
    group = first_a.shape[0]

    def rows_of(which):
        return pl.ds(pl.multiple_of(which * half, half), half)

    def peer(offset):
        return lax.rem(chip + offset, chips) * 2 + core

    def source_of(offset):
        return lax.rem(chip + chips - offset, chips)

    def a_copy(slot):
        return pltpu.make_async_copy(stats.at[0, slot], a_buf.at[slot - group], a_sem.at[slot - group])

    def x_copy(slot):
        return pltpu.make_async_copy(starts.at[0, slot], x_buf.at[slot - group], x_sem.at[slot - group])

    def g_copy(owner):
        return pltpu.make_async_copy(grads.at[owner], g_buf.at[owner], g_sem.at[owner])

    def send(source, place, target, send_sem, recv_sem):
        return pltpu.make_async_remote_copy(
            src_ref=source, dst_ref=place, send_sem=send_sem, recv_sem=recv_sem,
            device_id=target, device_id_type=MESH)

    def p_copy(which, slot, early=False):
        block = low.at[which, slot] if early else high.at[which, slot - group]
        return send(block, block, {"mp": partner}, p_send.at[slot], p_recv.at[slot])

    def first_copy(offset):
        return send(low.at[core, 0], landed.at[offset - 1, core], {"mp": peer(offset)},
                    y_send.at[offset - 1, 0], y_recv.at[offset - 1, 0])

    def first_forward(offset, which):
        block = landed.at[offset - 1, which]
        return send(block, block, {"mp": partner}, f_send.at[offset - 1, 0], f_recv.at[offset - 1, 0])

    def y_copy(offset, position):
        return send(staged.at[position - 2], landed.at[offset - 1, position, rows_of(core)], {"mp": peer(offset)},
                    y_send.at[offset - 1, position - 1], y_recv.at[offset - 1, position - 1])

    def forward(offset, position, which):
        block = landed.at[offset - 1, position, rows_of(which)]
        return send(block, block, {"mp": partner}, f_send.at[offset - 1, position - 1], f_recv.at[offset - 1, position - 1])

    def relay_copy(number, which):
        at_core, at_slot = relayed_block(number)
        return send(low.at[at_core, at_slot, rows_of(which)], relayed.at[number], {"dp": beside, "mp": 2 * chip + which},
                    r_send.at[number, which], r_recv.at[number])

    def back_copy(offset, number):
        return send(landed.at[offset - 1, window + number, rows_of(core)], returned.at[offset - 1, number, rows_of(core)],
                    {"dp": beside, "mp": me}, b_send.at[offset - 1, number], b_recv.at[offset - 1, number])

    def back_forward(offset, number, which):
        block = returned.at[offset - 1, number, rows_of(which)]
        return send(block, block, {"mp": partner}, h_send.at[offset - 1, number], h_recv.at[offset - 1, number])

    barrier = pltpu.get_barrier_semaphore()
    pl.semaphore_signal(barrier, inc=1, device_id={"mp": partner}, device_id_type=MESH)
    for offset in range(1, chips):
        pl.semaphore_signal(barrier, inc=1, device_id={"mp": peer(offset)}, device_id_type=MESH)
    for which in range(2):
        pl.semaphore_signal(barrier, inc=1, device_id={"dp": beside, "mp": 2 * chip + which}, device_id_type=MESH)
    greeted = chips + 2
    for slot in range(group, slots):
        x_copy(slot).start()
        a_copy(slot).start()

    live_count = counts[me, data]
    mine, theirs = Load(counts, chip, data, positions, spared), Load(counts, chip, beside, positions, spared)

    def compute(batch, a_blocks, x_blocks):
        found = newton_roots(a_blocks, x_blocks)
        for slot, root in zip(batch, found):
            live = jnp.full(root.shape, slot, jnp.int32) < live_count
            yield slot, jnp.where(live, root, 0.0).astype(jnp.bfloat16)

    for slot, root in compute(range(group), [first_a[at] for at in range(group)], [first_x[at] for at in range(group)]):
        low[core, slot] = root
    pl.semaphore_wait(barrier, greeted)
    for offset in range(1, chips):
        first_copy(offset).start()
    for number in range(relays):
        @pl.when(core == relayed_block(number)[0])
        def _():
            for which in range(2):
                relay_copy(number, which).start()
    for slot in range(group):
        p_copy(core, slot, True).start()
    for owner in range(members):
        g_copy(owner).start()

    @pl.loop(1, slots // group)
    def _(turn):
        batch = [turn * group + at for at in range(group)]
        for slot in batch:
            x_copy(slot).wait()
            a_copy(slot).wait()
        for slot, root in compute(batch, [a_buf[slot - group] for slot in batch], [x_buf[slot - group] for slot in batch]):
            high[core, slot - group] = root
        for slot in batch:
            p_copy(core, slot).start()

    def launch(position, filled, early=False, taken=None):
        at_core, at_slot = packed_at(kept_index(position - filled, mine.excess), mine.first, mine.second, slots)
        value = low[at_core, jnp.minimum(at_slot, group - 1), rows_of(core)]
        if not early:
            later = high[at_core, jnp.maximum(at_slot - group, 0), rows_of(core)]
            value = lax.select_n(at_slot >= group, value, later)
        if taken is not None:
            value = lax.select_n(taken < theirs.excess, value, relayed[taken])
        staged[position - 2] = value
        for offset in range(1, chips):
            y_copy(offset, position).start()

    def near_apply(which):
        for at in range(group):
            near[which, at] = dot(low[which, at], g_buf[2 * chip + which, at]).astype(near.dtype)

        @pl.loop(1, slots // group)
        def _(turn):
            for at in range(group):
                slot = turn * group + at
                near[which, slot] = dot(high[which, slot - group], g_buf[2 * chip + which, slot]).astype(near.dtype)

    def receive(early):
        @pl.loop(0 if early else group, group if early else slots)
        def _(slot):
            p_copy(other, slot, early).wait_recv()

    receive(True)
    for position in range(2, window):
        launch(position, 0, True)
    for number in range(relays):
        position = window + number
        if position == group + 1:
            for owner in range(members):
                g_copy(owner).wait()
            near_apply(core)
            receive(False)
        relay_copy(number, core).wait_recv()
        launch(position, theirs.excess, position <= group, number)

    @pl.loop(window + relays, capacity(positions, spared, chip, data))
    def _(position):
        launch(position, theirs.excess)

    near_apply(other)
    last = far.shape[1] - 1
    for at in range(chips - 1):
        far[at, last] = jnp.zeros(far.shape[2:], far.dtype)

    loads = {offset: [Load(counts, source_of(offset), at, positions, spared) for at in (data, beside)]
             for offset in range(1, chips)}

    def arrive(offset, kind, number):
        if kind == "first":
            first_copy(offset).wait_recv()
            first_forward(offset, core).start()
        elif kind == "position":
            y_copy(offset, number).wait_recv()
            forward(offset, number, core).start()
            if window <= number < window + relays:
                back_copy(offset, number - window).start()
        else:
            back_copy(offset, number).wait_recv()
            back_forward(offset, number, core).start()

    def apply(offset, kind, number):
        source = source_of(offset)
        at = offset - 1
        if kind == "first":
            first_forward(offset, other).wait_recv()
            for which in range(2):
                far[at, which] = dot(landed[at, which], g_buf[2 * source + which, 0]).astype(far.dtype)
        elif kind == "position":
            forward(offset, number, other).wait_recv()
            own, side = loads[offset]
            index = kept_index(number - side.excess if number >= window else number, own.excess)
            at_core, at_slot = packed_at(index, own.first, own.second, slots)
            far[at, number] = dot(landed[at, number], g_buf[2 * source + at_core, at_slot]).astype(far.dtype)
        else:
            back_forward(offset, number, other).wait_recv()
            at_core, at_slot = relayed_block(number)
            far[at, positions + number] = dot(returned[at, number], g_buf[2 * source + at_core, at_slot]).astype(far.dtype)

    events = [(2.0, "first", 0)]
    events += [(position + 1.0, "position", position) for position in range(2, positions)]
    events += [(window + number + BACK, "back", number) for number in range(relays)]
    events = [event[1:] for event in sorted(events)]
    def where_sent(sender, position):
        if spared == 0 or position < positions - 2:
            return lambda run: run()
        return pl.when(position < capacity(positions, spared, sender, data))

    def at_each_offset(step, kind, number):
        for offset in range(1, chips):
            when = where_sent(source_of(offset), number) if kind == "position" else (lambda run: run())
            when(functools.partial(step, offset, kind, number))

    at_each_offset(arrive, *events[0])
    for before, now in zip(events, events[1:]):
        at_each_offset(arrive, *now)
        at_each_offset(apply, *before)

    @pl.loop(0, group)
    def _(slot):
        p_copy(core, slot, True).wait_send()

    @pl.loop(group, slots)
    def _(slot):
        p_copy(core, slot).wait_send()

    for number in range(relays):
        @pl.when(core == relayed_block(number)[0])
        def _():
            for which in range(2):
                relay_copy(number, which).wait_send()

    def sent(offset, kind, number):
        if kind == "first":
            first_copy(offset).wait_send()
        elif kind == "position":
            y_copy(offset, number).wait_send()
        else:
            back_copy(offset, number).wait_send()

    def forwarded(offset, kind, number):
        if kind == "first":
            first_forward(offset, core).wait_send()
        elif kind == "position":
            forward(offset, number, core).wait_send()
        else:
            back_forward(offset, number, core).wait_send()

    for kind, number in events:
        for offset in range(1, chips):
            when = where_sent(chip, number) if kind == "position" else (lambda run: run())
            when(functools.partial(sent, offset, kind, number))
    for event in events[:-1]:
        at_each_offset(forwarded, *event)
    at_each_offset(apply, *events[-1])
    at_each_offset(forwarded, *events[-1])


def placing_kernel(members, positions, spared, relays, window, counts, near, far, out, near_sem, far_sem):
    me = lax.axis_index("mp")
    data = lax.axis_index("dp")
    chips = members // 2
    chip = me // 2
    slots = near.shape[1]

    def near_copy(which):
        return pltpu.make_async_copy(near.at[which], out.at[2 * chip + which], near_sem.at[which])

    for which in range(2):
        near_copy(which).start()
    copies = []
    for offset in range(1, chips):
        source = lax.rem(chip + chips - offset, chips)
        own, side = (Load(counts, source, at, positions, spared) for at in (data, neighbour_of(data)))
        both = jnp.minimum(own.first, own.second)
        for which in range(2):
            for slot in range(slots):
                index = jnp.where(slot < both, 2 * slot + which, slot + both)
                odd = lax.rem(index, 2)
                near_start = index <= 2 * own.excess + 1
                kept = jnp.where(index < 2, index, jnp.where(near_start, lax.div(index + 1, 2), index - own.excess))
                place = jnp.where(kept < window, kept, kept + side.excess)
                passed = (index >= 2) & near_start & (odd == 0)
                place = jnp.where(passed, positions + lax.div(index, 2) - 1, place)
                place = jnp.where(slot < (own.first, own.second)[which], place, far.shape[1] - 1)
                copies.append(pltpu.make_async_copy(
                    far.at[offset - 1, place], out.at[2 * source + which, slot], far_sem.at[offset - 1, which, slot]))
                copies[-1].start()
    for which in range(2):
        near_copy(which).wait()
    for copy in copies:
        copy.wait()


def exchange(members, number, positions, spared, relays, window, counts, first_a, first_x, stats, prev_roots, grads):
    slots, size = stats.shape[1], stats.shape[2]
    chips = members // 2
    square = (size, size)
    near = (2, slots) + square
    far = (chips - 1, positions + relays + 1) + square
    group = first_a.shape[0]
    kept = grads.dtype.itemsize * size * size * (near[0] * near[1] + far[0] * far[1])
    kept += 2 * first_a.size * first_a.dtype.itemsize
    semaphores = pltpu.SemaphoreType.DMA
    steps, backs = (chips - 1, positions - 1), (chips - 1, relays)
    near, far = pl.pallas_call(
        functools.partial(kernel, members, positions, spared, relays, window),
        out_shape=(pltpu.VMEM(near, grads.dtype), pltpu.VMEM(far, grads.dtype)),
        in_specs=[pl.BlockSpec(memory_space=space)
                  for space in (pltpu.SMEM, pltpu.VMEM, pltpu.VMEM, pltpu.HBM, pltpu.HBM, pltpu.HBM)],
        out_specs=(pl.BlockSpec(memory_space=pltpu.VMEM), pl.BlockSpec(memory_space=pltpu.VMEM)),
        scratch_shapes=[
            pltpu.VMEM((slots - group,) + square, jnp.float32),
            pltpu.VMEM((slots - group,) + square, jnp.float32),
            pltpu.VMEM(grads.shape, grads.dtype),
            pltpu.VMEM((2, group) + square, jnp.bfloat16),
            pltpu.VMEM((2, slots - group) + square, jnp.bfloat16),
            pltpu.VMEM((positions - 2, size // 2, size), jnp.bfloat16),
            pltpu.VMEM((chips - 1, positions) + square, jnp.bfloat16),
            pltpu.VMEM((relays, size // 2, size), jnp.bfloat16),
            pltpu.VMEM((chips - 1, relays) + square, jnp.bfloat16),
            semaphores((slots - group,)),
            semaphores((slots - group,)),
            semaphores((members,)),
            semaphores(steps),
            semaphores(steps),
            semaphores((slots,)),
            semaphores((slots,)),
            semaphores(steps),
            semaphores(steps),
            semaphores((relays, 2)),
            semaphores((relays,)),
            semaphores(backs),
            semaphores(backs),
            semaphores(backs),
            semaphores(backs),
        ],
        compiler_params=pltpu.CompilerParams(
            collective_id=number, has_side_effects=True, vmem_limit_bytes=VMEM_BYTES - kept),
    )(counts, first_a, first_x, stats, prev_roots, grads)
    return pl.pallas_call(
        functools.partial(placing_kernel, members, positions, spared, relays, window),
        out_shape=pltpu.HBM(grads.shape, grads.dtype),
        in_specs=[
            pl.BlockSpec(memory_space=pltpu.SMEM),
            pl.BlockSpec(memory_space=pltpu.VMEM),
            pl.BlockSpec(memory_space=pltpu.VMEM),
        ],
        out_specs=pl.BlockSpec(memory_space=pltpu.HBM),
        scratch_shapes=[
            semaphores((2,)),
            semaphores((chips - 1, 2, slots)),
        ],
        compiler_params=pltpu.CompilerParams(vmem_limit_bytes=1 << 20),
    )(counts, near, far)


def local(members, stats, prev_roots, counts, grads):
    slots = stats.shape[1]
    sizes = list(range(slots + 2, slots + 6)) + [2 * slots]
    first = (GROUP,) + stats.shape[2:]
    semaphores = pltpu.SemaphoreType.DMA
    choice, table, first_a, first_x = pl.pallas_call(
        functools.partial(opening_kernel, sizes, RELAYS, slots),
        out_shape=(pltpu.SMEM((1,), jnp.int32), pltpu.SMEM(counts.shape, counts.dtype),
                   pltpu.VMEM(first, stats.dtype), pltpu.VMEM(first, stats.dtype)),
        in_specs=[pl.BlockSpec(memory_space=pltpu.HBM)] * 3,
        out_specs=tuple(pl.BlockSpec(memory_space=space) for space in (pltpu.SMEM, pltpu.SMEM, pltpu.VMEM, pltpu.VMEM)),
        scratch_shapes=[semaphores, semaphores((GROUP,)), semaphores((GROUP,))],
        compiler_params=pltpu.CompilerParams(vmem_limit_bytes=1 << 20),
    )(pltpu.with_memory_space_constraint(counts, pltpu.HBM), stats, prev_roots)
    branches = [functools.partial(exchange, members, number, size, int(size != sizes[-1]), RELAYS, WINDOW)
                for number, size in enumerate(sizes)]
    return lax.switch(choice[0], branches, table, first_a, first_x, stats, prev_roots, grads)


def solution(mesh):
    return jax.shard_map(
        functools.partial(local, mesh.shape["mp"]),
        mesh=mesh,
        in_specs=(
            P("mp", "dp", None, None),
            P("mp", "dp", None, None),
            P(),
            P(None, "dp", None, "mp"),
        ),
        out_specs=P(None, "dp", None, "mp"),
        check_vma=False,
    )
```

```python
import functools

import jax
import jax.numpy as jnp
from jax import lax
from jax.experimental import pallas as pl
from jax.experimental.pallas import tpu as pltpu
from jax.sharding import PartitionSpec as P

VMEM_BYTES = 67043328 - 65536
MESH = pl.DeviceIdType.MESH
RELAYS = 3
WINDOW = 3
BACK = 3.6
GROUP = 4


def dot(left, right):
    return jnp.dot(left.astype(jnp.bfloat16), right.astype(jnp.bfloat16), preferred_element_type=jnp.float32)


def shifted_squares(parts):
    return [2.0 * part + dot(part, part) for part in parts]


def newton_roots(statistics, initials):
    size = initials[0].shape[-1]
    rows = lax.broadcasted_iota(jnp.int32, (size, size), 0)
    columns = lax.broadcasted_iota(jnp.int32, (size, size), 1)
    identity = jnp.where(rows == columns, 1.0, 0.0).astype(jnp.float32)
    fourths = shifted_squares(shifted_squares([initial - identity for initial in initials]))
    moments = [statistic + dot(fourth, statistic) for fourth, statistic in zip(fourths, statistics)]
    changes = [0.25 * (identity - moment) for moment in moments]
    estimates = [initial + dot(initial, change) for initial, change in zip(initials, changes)]
    fourths = shifted_squares(shifted_squares(changes))
    moments = [moment + dot(fourth, moment) for fourth, moment in zip(fourths, moments)]
    changes = [0.25 * (identity - moment) for moment in moments]
    return [estimate + dot(estimate, change) for estimate, change in zip(estimates, changes)]


def packed_at(index, first, second, slots):
    both = jnp.minimum(first, second)
    paired = index < 2 * both
    slot = jnp.where(paired, lax.div(index, 2), index - both)
    core = jnp.where(paired, lax.rem(index, 2), jnp.where(first > second, 0, 1))
    return core, jnp.clip(slot, 0, slots - 1)


def neighbour_of(data):
    return data + 1 - 2 * lax.rem(data, 2)


def relayed_block(number):
    return 0, 1 + number


def kept_index(number, excess):
    number = jnp.maximum(number, 2)
    return jnp.minimum(2 * number - 1, number + excess)


def capacity(positions, spared, chip, data):
    return positions - spared * ((chip > 0).astype(jnp.int32) + (data == 0).astype(jnp.int32))


class Load:
    def __init__(self, counts, chip, data, positions, spared):
        self.first, self.second = counts[2 * chip, data], counts[2 * chip + 1, data]
        self.excess = jnp.maximum(self.first + self.second - capacity(positions, spared, chip, data), 0)


def opening_kernel(sizes, relays, slots, count_table, stats, starts, choice, counts, first_a, first_x, count_sem, a_sem, x_sem):
    group = first_a.shape[0]
    copies = [pltpu.make_async_copy(count_table, counts, count_sem)]
    copies += [pltpu.make_async_copy(starts.at[0, slot], first_x.at[slot], x_sem.at[slot]) for slot in range(group)]
    copies += [pltpu.make_async_copy(stats.at[0, slot], first_a.at[slot], a_sem.at[slot]) for slot in range(group)]
    for copy in copies:
        copy.start()
    copies[0].wait()
    members, workers = counts.shape
    need = jnp.int32(0)
    for chip in range(members // 2):
        for data in range(0, workers, 2):
            pair = [counts[2 * chip, at] + counts[2 * chip + 1, at] for at in (data, data + 1)]
            fewer = int(chip > 0)
            spared = int(data == 0)
            least = lax.div(pair[0] + pair[1] + 1 + spared, 2) + fewer
            most = jnp.maximum(pair[0] + spared, pair[1]) + fewer
            least = jnp.maximum(least, most - relays)
            least = jnp.where(most - (relays - 1) > sizes[0], jnp.maximum(least, sizes[1]), least)
            if sizes[0] - fewer - spared <= slots:
                both = jnp.minimum(counts[2 * chip, data], counts[2 * chip + 1, data])
                over = pair[0] - (sizes[0] - fewer - spared)
                least = jnp.where((over > 0) & (both <= over), jnp.maximum(least, sizes[1]), least)
            need = jnp.maximum(need, least)
    choice[0] = sum((need > size).astype(jnp.int32) for size in sizes[:-1])
    for copy in copies[1:]:
        copy.wait()


def kernel(members, positions, spared, relays, window, counts, first_a, first_x, stats, starts, grads, near, far, a_buf, x_buf, g_buf, low, high, staged, landed, relayed, returned, a_sem, x_sem, g_sem, y_send, y_recv, p_send, p_recv,
           f_send, f_recv, r_send, r_recv, b_send, b_recv, h_send, h_recv):
    me = lax.axis_index("mp")
    data = lax.axis_index("dp")
    slots, size = stats.shape[1], stats.shape[2]
    chips = members // 2
    core = lax.rem(me, 2)
    chip = me // 2
    other = 1 - core
    partner = 2 * chip + other
    beside = neighbour_of(data)
    half = size // 2
    group = first_a.shape[0]

    def rows_of(which):
        return pl.ds(pl.multiple_of(which * half, half), half)

    def peer(offset):
        return lax.rem(chip + offset, chips) * 2 + core

    def source_of(offset):
        return lax.rem(chip + chips - offset, chips)

    def a_copy(slot):
        return pltpu.make_async_copy(stats.at[0, slot], a_buf.at[slot - group], a_sem.at[slot - group])

    def x_copy(slot):
        return pltpu.make_async_copy(starts.at[0, slot], x_buf.at[slot - group], x_sem.at[slot - group])

    def g_copy(owner):
        return pltpu.make_async_copy(grads.at[owner], g_buf.at[owner], g_sem.at[owner])

    def send(source, place, target, send_sem, recv_sem):
        return pltpu.make_async_remote_copy(
            src_ref=source, dst_ref=place, send_sem=send_sem, recv_sem=recv_sem,
            device_id=target, device_id_type=MESH)

    def p_copy(which, slot, early=False):
        block = low.at[which, slot] if early else high.at[which, slot - group]
        return send(block, block, {"mp": partner}, p_send.at[slot], p_recv.at[slot])

    def first_copy(offset):
        return send(low.at[core, 0], landed.at[offset - 1, core], {"mp": peer(offset)},
                    y_send.at[offset - 1, 0], y_recv.at[offset - 1, 0])

    def first_forward(offset, which):
        block = landed.at[offset - 1, which]
        return send(block, block, {"mp": partner}, f_send.at[offset - 1, 0], f_recv.at[offset - 1, 0])

    def y_copy(offset, position):
        return send(staged.at[position - 2], landed.at[offset - 1, position, rows_of(core)], {"mp": peer(offset)},
                    y_send.at[offset - 1, position - 1], y_recv.at[offset - 1, position - 1])

    def forward(offset, position, which):
        block = landed.at[offset - 1, position, rows_of(which)]
        return send(block, block, {"mp": partner}, f_send.at[offset - 1, position - 1], f_recv.at[offset - 1, position - 1])

    def relay_copy(number, which):
        at_core, at_slot = relayed_block(number)
        return send(low.at[at_core, at_slot, rows_of(which)], relayed.at[number], {"dp": beside, "mp": 2 * chip + which},
                    r_send.at[number, which], r_recv.at[number])

    def back_copy(offset, number):
        return send(landed.at[offset - 1, window + number, rows_of(core)], returned.at[offset - 1, number, rows_of(core)],
                    {"dp": beside, "mp": me}, b_send.at[offset - 1, number], b_recv.at[offset - 1, number])

    def back_forward(offset, number, which):
        block = returned.at[offset - 1, number, rows_of(which)]
        return send(block, block, {"mp": partner}, h_send.at[offset - 1, number], h_recv.at[offset - 1, number])

    barrier = pltpu.get_barrier_semaphore()
    pl.semaphore_signal(barrier, inc=1, device_id={"mp": partner}, device_id_type=MESH)
    for offset in range(1, chips):
        pl.semaphore_signal(barrier, inc=1, device_id={"mp": peer(offset)}, device_id_type=MESH)
    for which in range(2):
        pl.semaphore_signal(barrier, inc=1, device_id={"dp": beside, "mp": 2 * chip + which}, device_id_type=MESH)
    greeted = chips + 2
    for slot in range(group, slots):
        x_copy(slot).start()
        a_copy(slot).start()

    live_count = counts[me, data]
    mine, theirs = Load(counts, chip, data, positions, spared), Load(counts, chip, beside, positions, spared)

    def compute(batch, a_blocks, x_blocks):
        found = newton_roots(a_blocks, x_blocks)
        for slot, root in zip(batch, found):
            live = jnp.full(root.shape, slot, jnp.int32) < live_count
            yield slot, jnp.where(live, root, 0.0).astype(jnp.bfloat16)

    for slot, root in compute(range(group), [first_a[at] for at in range(group)], [first_x[at] for at in range(group)]):
        low[core, slot] = root
    pl.semaphore_wait(barrier, greeted)
    for offset in range(1, chips):
        first_copy(offset).start()
    for number in range(relays):
        @pl.when(core == relayed_block(number)[0])
        def _():
            for which in range(2):
                relay_copy(number, which).start()
    for slot in range(group):
        p_copy(core, slot, True).start()
    for owner in range(members):
        g_copy(owner).start()

    @pl.loop(1, slots // group)
    def _(turn):
        batch = [turn * group + at for at in range(group)]
        for slot in batch:
            x_copy(slot).wait()
            a_copy(slot).wait()
        for slot, root in compute(batch, [a_buf[slot - group] for slot in batch], [x_buf[slot - group] for slot in batch]):
            high[core, slot - group] = root
        for slot in batch:
            p_copy(core, slot).start()

    def launch(position, filled, early=False, taken=None):
        at_core, at_slot = packed_at(kept_index(position - filled, mine.excess), mine.first, mine.second, slots)
        value = low[at_core, jnp.minimum(at_slot, group - 1), rows_of(core)]
        if not early:
            later = high[at_core, jnp.maximum(at_slot - group, 0), rows_of(core)]
            value = lax.select_n(at_slot >= group, value, later)
        if taken is not None:
            value = lax.select_n(taken < theirs.excess, value, relayed[taken])
        staged[position - 2] = value
        for offset in range(1, chips):
            y_copy(offset, position).start()

    def near_apply(which):
        for at in range(group):
            near[which, at] = dot(low[which, at], g_buf[2 * chip + which, at]).astype(near.dtype)

        @pl.loop(1, slots // group)
        def _(turn):
            for at in range(group):
                slot = turn * group + at
                near[which, slot] = dot(high[which, slot - group], g_buf[2 * chip + which, slot]).astype(near.dtype)

    def receive(early):
        @pl.loop(0 if early else group, group if early else slots)
        def _(slot):
            p_copy(other, slot, early).wait_recv()

    receive(True)
    for position in range(2, window):
        launch(position, 0, True)
    for number in range(relays):
        position = window + number
        if position == min(group + 1, window + relays - 1):
            for owner in range(members):
                g_copy(owner).wait()
            near_apply(core)
            receive(False)
        relay_copy(number, core).wait_recv()
        launch(position, theirs.excess, position <= group, number)

    @pl.loop(window + relays, capacity(positions, spared, chip, data))
    def _(position):
        launch(position, theirs.excess)

    near_apply(other)
    last = far.shape[1] - 1
    for at in range(chips - 1):
        far[at, last] = jnp.zeros(far.shape[2:], far.dtype)

    loads = {offset: [Load(counts, source_of(offset), at, positions, spared) for at in (data, beside)]
             for offset in range(1, chips)}

    def arrive(offset, kind, number):
        if kind == "first":
            first_copy(offset).wait_recv()
            first_forward(offset, core).start()
        elif kind == "position":
            y_copy(offset, number).wait_recv()
            forward(offset, number, core).start()
            if window <= number < window + relays:
                back_copy(offset, number - window).start()
        else:
            back_copy(offset, number).wait_recv()
            back_forward(offset, number, core).start()

    def apply(offset, kind, number):
        source = source_of(offset)
        at = offset - 1
        if kind == "first":
            first_forward(offset, other).wait_recv()
            for which in range(2):
                far[at, which] = dot(landed[at, which], g_buf[2 * source + which, 0]).astype(far.dtype)
        elif kind == "position":
            forward(offset, number, other).wait_recv()
            own, side = loads[offset]
            index = kept_index(number - side.excess if number >= window else number, own.excess)
            at_core, at_slot = packed_at(index, own.first, own.second, slots)
            far[at, number] = dot(landed[at, number], g_buf[2 * source + at_core, at_slot]).astype(far.dtype)
        else:
            back_forward(offset, number, other).wait_recv()
            at_core, at_slot = relayed_block(number)
            far[at, positions + number] = dot(returned[at, number], g_buf[2 * source + at_core, at_slot]).astype(far.dtype)

    events = [(2.0, "first", 0)]
    events += [(position + 1.0, "position", position) for position in range(2, positions)]
    events += [(window + number + BACK, "back", number) for number in range(relays)]
    events = [event[1:] for event in sorted(events)]
    def where_sent(sender, position):
        if spared == 0 or position < positions - 2:
            return lambda run: run()
        return pl.when(position < capacity(positions, spared, sender, data))

    def at_each_offset(step, kind, number):
        for offset in range(1, chips):
            when = where_sent(source_of(offset), number) if kind == "position" else (lambda run: run())
            when(functools.partial(step, offset, kind, number))

    at_each_offset(arrive, *events[0])
    for before, now in zip(events, events[1:]):
        at_each_offset(arrive, *now)
        at_each_offset(apply, *before)

    @pl.loop(0, group)
    def _(slot):
        p_copy(core, slot, True).wait_send()

    @pl.loop(group, slots)
    def _(slot):
        p_copy(core, slot).wait_send()

    for number in range(relays):
        @pl.when(core == relayed_block(number)[0])
        def _():
            for which in range(2):
                relay_copy(number, which).wait_send()

    def sent(offset, kind, number):
        if kind == "first":
            first_copy(offset).wait_send()
        elif kind == "position":
            y_copy(offset, number).wait_send()
        else:
            back_copy(offset, number).wait_send()

    def forwarded(offset, kind, number):
        if kind == "first":
            first_forward(offset, core).wait_send()
        elif kind == "position":
            forward(offset, number, core).wait_send()
        else:
            back_forward(offset, number, core).wait_send()

    for kind, number in events:
        for offset in range(1, chips):
            when = where_sent(chip, number) if kind == "position" else (lambda run: run())
            when(functools.partial(sent, offset, kind, number))
    for event in events[:-1]:
        at_each_offset(forwarded, *event)
    at_each_offset(apply, *events[-1])
    at_each_offset(forwarded, *events[-1])


def placing_kernel(members, positions, spared, relays, window, counts, near, far, out, near_sem, far_sem):
    me = lax.axis_index("mp")
    data = lax.axis_index("dp")
    chips = members // 2
    chip = me // 2
    slots = near.shape[1]

    def near_copy(which):
        return pltpu.make_async_copy(near.at[which], out.at[2 * chip + which], near_sem.at[which])

    for which in range(2):
        near_copy(which).start()
    copies = []
    for offset in range(1, chips):
        source = lax.rem(chip + chips - offset, chips)
        own, side = (Load(counts, source, at, positions, spared) for at in (data, neighbour_of(data)))
        both = jnp.minimum(own.first, own.second)
        for which in range(2):
            for slot in range(slots):
                index = jnp.where(slot < both, 2 * slot + which, slot + both)
                odd = lax.rem(index, 2)
                near_start = index <= 2 * own.excess + 1
                kept = jnp.where(index < 2, index, jnp.where(near_start, lax.div(index + 1, 2), index - own.excess))
                place = jnp.where(kept < window, kept, kept + side.excess)
                passed = (index >= 2) & near_start & (odd == 0)
                place = jnp.where(passed, positions + lax.div(index, 2) - 1, place)
                place = jnp.where(slot < (own.first, own.second)[which], place, far.shape[1] - 1)
                copies.append(pltpu.make_async_copy(
                    far.at[offset - 1, place], out.at[2 * source + which, slot], far_sem.at[offset - 1, which, slot]))
                copies[-1].start()
    for which in range(2):
        near_copy(which).wait()
    for copy in copies:
        copy.wait()


def exchange(members, number, positions, spared, relays, window, counts, first_a, first_x, stats, prev_roots, grads):
    slots, size = stats.shape[1], stats.shape[2]
    chips = members // 2
    square = (size, size)
    near = (2, slots) + square
    far = (chips - 1, positions + relays + 1) + square
    group = first_a.shape[0]
    kept = grads.dtype.itemsize * size * size * (near[0] * near[1] + far[0] * far[1])
    kept += 2 * first_a.size * first_a.dtype.itemsize
    semaphores = pltpu.SemaphoreType.DMA
    steps, backs = (chips - 1, positions - 1), (chips - 1, relays)
    near, far = pl.pallas_call(
        functools.partial(kernel, members, positions, spared, relays, window),
        out_shape=(pltpu.VMEM(near, grads.dtype), pltpu.VMEM(far, grads.dtype)),
        in_specs=[pl.BlockSpec(memory_space=space)
                  for space in (pltpu.SMEM, pltpu.VMEM, pltpu.VMEM, pltpu.HBM, pltpu.HBM, pltpu.HBM)],
        out_specs=(pl.BlockSpec(memory_space=pltpu.VMEM), pl.BlockSpec(memory_space=pltpu.VMEM)),
        scratch_shapes=[
            pltpu.VMEM((slots - group,) + square, jnp.float32),
            pltpu.VMEM((slots - group,) + square, jnp.float32),
            pltpu.VMEM(grads.shape, grads.dtype),
            pltpu.VMEM((2, group) + square, jnp.bfloat16),
            pltpu.VMEM((2, slots - group) + square, jnp.bfloat16),
            pltpu.VMEM((positions - 2, size // 2, size), jnp.bfloat16),
            pltpu.VMEM((chips - 1, positions) + square, jnp.bfloat16),
            pltpu.VMEM((relays, size // 2, size), jnp.bfloat16),
            pltpu.VMEM((chips - 1, relays) + square, jnp.bfloat16),
            semaphores((slots - group,)),
            semaphores((slots - group,)),
            semaphores((members,)),
            semaphores(steps),
            semaphores(steps),
            semaphores((slots,)),
            semaphores((slots,)),
            semaphores(steps),
            semaphores(steps),
            semaphores((relays, 2)),
            semaphores((relays,)),
            semaphores(backs),
            semaphores(backs),
            semaphores(backs),
            semaphores(backs),
        ],
        compiler_params=pltpu.CompilerParams(
            collective_id=number, has_side_effects=True, vmem_limit_bytes=VMEM_BYTES - kept),
    )(counts, first_a, first_x, stats, prev_roots, grads)
    return pl.pallas_call(
        functools.partial(placing_kernel, members, positions, spared, relays, window),
        out_shape=pltpu.HBM(grads.shape, grads.dtype),
        in_specs=[
            pl.BlockSpec(memory_space=pltpu.SMEM),
            pl.BlockSpec(memory_space=pltpu.VMEM),
            pl.BlockSpec(memory_space=pltpu.VMEM),
        ],
        out_specs=pl.BlockSpec(memory_space=pltpu.HBM),
        scratch_shapes=[
            semaphores((2,)),
            semaphores((chips - 1, 2, slots)),
        ],
        compiler_params=pltpu.CompilerParams(vmem_limit_bytes=1 << 20),
    )(counts, near, far)


def local(members, stats, prev_roots, counts, grads):
    slots = stats.shape[1]
    sizes = list(range(slots + 2, slots + 6)) + [2 * slots]
    first = (GROUP,) + stats.shape[2:]
    semaphores = pltpu.SemaphoreType.DMA
    choice, table, first_a, first_x = pl.pallas_call(
        functools.partial(opening_kernel, sizes, RELAYS, slots),
        out_shape=(pltpu.SMEM((1,), jnp.int32), pltpu.SMEM(counts.shape, counts.dtype),
                   pltpu.VMEM(first, stats.dtype), pltpu.VMEM(first, stats.dtype)),
        in_specs=[pl.BlockSpec(memory_space=pltpu.HBM)] * 3,
        out_specs=tuple(pl.BlockSpec(memory_space=space) for space in (pltpu.SMEM, pltpu.SMEM, pltpu.VMEM, pltpu.VMEM)),
        scratch_shapes=[semaphores, semaphores((GROUP,)), semaphores((GROUP,))],
        compiler_params=pltpu.CompilerParams(vmem_limit_bytes=1 << 20),
    )(pltpu.with_memory_space_constraint(counts, pltpu.HBM), stats, prev_roots)
    branches = [functools.partial(exchange, members, number, size, int(size != sizes[-1]),
                                  RELAYS - int(number == 0), WINDOW)
                for number, size in enumerate(sizes)]
    return lax.switch(choice[0], branches, table, first_a, first_x, stats, prev_roots, grads)


def solution(mesh):
    return jax.shard_map(
        functools.partial(local, mesh.shape["mp"]),
        mesh=mesh,
        in_specs=(
            P("mp", "dp", None, None),
            P("mp", "dp", None, None),
            P(),
            P(None, "dp", None, "mp"),
        ),
        out_specs=P(None, "dp", None, "mp"),
        check_vma=False,
    )
```

```python
import functools

import jax
import jax.numpy as jnp
from jax import lax
from jax.experimental import pallas as pl
from jax.experimental.pallas import tpu as pltpu
from jax.sharding import PartitionSpec as P

VMEM_BYTES = 67043328 - 65536
MESH = pl.DeviceIdType.MESH
RELAYS = 3
WINDOW = 3
BACK = 3.6
GROUP = 4


def dot(left, right):
    return jnp.dot(left.astype(jnp.bfloat16), right.astype(jnp.bfloat16), preferred_element_type=jnp.float32)


def shifted_squares(parts):
    return [2.0 * part + dot(part, part) for part in parts]


def newton_roots(statistics, initials):
    size = initials[0].shape[-1]
    rows = lax.broadcasted_iota(jnp.int32, (size, size), 0)
    columns = lax.broadcasted_iota(jnp.int32, (size, size), 1)
    identity = jnp.where(rows == columns, 1.0, 0.0).astype(jnp.float32)
    fourths = shifted_squares(shifted_squares([initial - identity for initial in initials]))
    moments = [statistic + dot(fourth, statistic) for fourth, statistic in zip(fourths, statistics)]
    changes = [0.25 * (identity - moment) for moment in moments]
    estimates = [initial + dot(initial, change) for initial, change in zip(initials, changes)]
    fourths = shifted_squares(shifted_squares(changes))
    moments = [moment + dot(fourth, moment) for fourth, moment in zip(fourths, moments)]
    changes = [0.25 * (identity - moment) for moment in moments]
    return [estimate + dot(estimate, change) for estimate, change in zip(estimates, changes)]


def packed_at(index, first, second, slots):
    both = jnp.minimum(first, second)
    paired = index < 2 * both
    slot = jnp.where(paired, lax.div(index, 2), index - both)
    core = jnp.where(paired, lax.rem(index, 2), jnp.where(first > second, 0, 1))
    return core, jnp.clip(slot, 0, slots - 1)


def neighbour_of(data):
    return data + 1 - 2 * lax.rem(data, 2)


def relayed_block(number):
    return 0, 1 + number


def kept_index(number, excess):
    number = jnp.maximum(number, 2)
    return jnp.minimum(2 * number - 1, number + excess)


def capacity(positions, spared, chip, data):
    return positions - spared[0] * (chip > 0).astype(jnp.int32) - spared[1] * (data == 0).astype(jnp.int32)


class Load:
    def __init__(self, counts, chip, data, positions, spared):
        self.first, self.second = counts[2 * chip, data], counts[2 * chip + 1, data]
        self.excess = jnp.maximum(self.first + self.second - capacity(positions, spared, chip, data), 0)


def opening_kernel(variants, slots, count_table, stats, starts, choice, counts, first_a, first_x, count_sem, a_sem, x_sem):
    group = first_a.shape[0]
    copies = [pltpu.make_async_copy(count_table, counts, count_sem)]
    copies += [pltpu.make_async_copy(starts.at[0, slot], first_x.at[slot], x_sem.at[slot]) for slot in range(group)]
    copies += [pltpu.make_async_copy(stats.at[0, slot], first_a.at[slot], a_sem.at[slot]) for slot in range(group)]
    for copy in copies:
        copy.start()
    copies[0].wait()
    members, workers = counts.shape
    picked = jnp.int32(len(variants) - 1)
    for number, (positions, spared, relays) in reversed(list(enumerate(variants[:-1]))):
        over = jnp.int32(0)
        for chip in range(members // 2):
            for data in range(0, workers, 2):
                total, room = 0, 0
                for at in (data, data + 1):
                    have = counts[2 * chip, at] + counts[2 * chip + 1, at]
                    most = positions - spared[0] * int(chip > 0) - spared[1] * int(at == 0)
                    over = jnp.maximum(over, have - most - relays)
                    if most <= slots:
                        both = jnp.minimum(counts[2 * chip, at], counts[2 * chip + 1, at])
                        over = jnp.where((have > most) & (both <= have - most), jnp.maximum(over, 1), over)
                    total, room = total + have, room + most
                over = jnp.maximum(over, total - room)
        picked = jnp.where(over > 0, picked, number)
    choice[0] = picked
    for copy in copies[1:]:
        copy.wait()


def kernel(members, positions, spared, relays, window, counts, first_a, first_x, stats, starts, grads, near, far, a_buf, x_buf, g_buf, low, high, staged, landed, relayed, returned, a_sem, x_sem, g_sem, y_send, y_recv, p_send, p_recv,
           f_send, f_recv, r_send, r_recv, b_send, b_recv, h_send, h_recv):
    me = lax.axis_index("mp")
    data = lax.axis_index("dp")
    slots, size = stats.shape[1], stats.shape[2]
    chips = members // 2
    core = lax.rem(me, 2)
    chip = me // 2
    other = 1 - core
    partner = 2 * chip + other
    beside = neighbour_of(data)
    half = size // 2
    group = first_a.shape[0]

    def rows_of(which):
        return pl.ds(pl.multiple_of(which * half, half), half)

    def peer(offset):
        return lax.rem(chip + offset, chips) * 2 + core

    def source_of(offset):
        return lax.rem(chip + chips - offset, chips)

    def a_copy(slot):
        return pltpu.make_async_copy(stats.at[0, slot], a_buf.at[slot - group], a_sem.at[slot - group])

    def x_copy(slot):
        return pltpu.make_async_copy(starts.at[0, slot], x_buf.at[slot - group], x_sem.at[slot - group])

    def g_copy(owner):
        return pltpu.make_async_copy(grads.at[owner], g_buf.at[owner], g_sem.at[owner])

    def send(source, place, target, send_sem, recv_sem):
        return pltpu.make_async_remote_copy(
            src_ref=source, dst_ref=place, send_sem=send_sem, recv_sem=recv_sem,
            device_id=target, device_id_type=MESH)

    def p_copy(which, slot, early=False):
        block = low.at[which, slot] if early else high.at[which, slot - group]
        return send(block, block, {"mp": partner}, p_send.at[slot], p_recv.at[slot])

    def first_copy(offset):
        return send(low.at[core, 0], landed.at[offset - 1, core], {"mp": peer(offset)},
                    y_send.at[offset - 1, 0], y_recv.at[offset - 1, 0])

    def first_forward(offset, which):
        block = landed.at[offset - 1, which]
        return send(block, block, {"mp": partner}, f_send.at[offset - 1, 0], f_recv.at[offset - 1, 0])

    def y_copy(offset, position):
        return send(staged.at[position - 2], landed.at[offset - 1, position, rows_of(core)], {"mp": peer(offset)},
                    y_send.at[offset - 1, position - 1], y_recv.at[offset - 1, position - 1])

    def forward(offset, position, which):
        block = landed.at[offset - 1, position, rows_of(which)]
        return send(block, block, {"mp": partner}, f_send.at[offset - 1, position - 1], f_recv.at[offset - 1, position - 1])

    def relay_copy(number, which):
        at_core, at_slot = relayed_block(number)
        return send(low.at[at_core, at_slot, rows_of(which)], relayed.at[number], {"dp": beside, "mp": 2 * chip + which},
                    r_send.at[number, which], r_recv.at[number])

    def back_copy(offset, number):
        return send(landed.at[offset - 1, window + number, rows_of(core)], returned.at[offset - 1, number, rows_of(core)],
                    {"dp": beside, "mp": me}, b_send.at[offset - 1, number], b_recv.at[offset - 1, number])

    def back_forward(offset, number, which):
        block = returned.at[offset - 1, number, rows_of(which)]
        return send(block, block, {"mp": partner}, h_send.at[offset - 1, number], h_recv.at[offset - 1, number])

    barrier = pltpu.get_barrier_semaphore()
    pl.semaphore_signal(barrier, inc=1, device_id={"mp": partner}, device_id_type=MESH)
    for offset in range(1, chips):
        pl.semaphore_signal(barrier, inc=1, device_id={"mp": peer(offset)}, device_id_type=MESH)
    for which in range(2):
        pl.semaphore_signal(barrier, inc=1, device_id={"dp": beside, "mp": 2 * chip + which}, device_id_type=MESH)
    greeted = chips + 2
    for slot in range(group, slots):
        x_copy(slot).start()
        a_copy(slot).start()

    live_count = counts[me, data]
    mine, theirs = Load(counts, chip, data, positions, spared), Load(counts, chip, beside, positions, spared)

    def compute(batch, a_blocks, x_blocks):
        found = newton_roots(a_blocks, x_blocks)
        for slot, root in zip(batch, found):
            live = jnp.full(root.shape, slot, jnp.int32) < live_count
            yield slot, jnp.where(live, root, 0.0).astype(jnp.bfloat16)

    for slot, root in compute(range(group), [first_a[at] for at in range(group)], [first_x[at] for at in range(group)]):
        low[core, slot] = root
    pl.semaphore_wait(barrier, greeted)
    for offset in range(1, chips):
        first_copy(offset).start()
    for number in range(relays):
        @pl.when(core == relayed_block(number)[0])
        def _():
            for which in range(2):
                relay_copy(number, which).start()
    for slot in range(group):
        p_copy(core, slot, True).start()
    for owner in range(members):
        g_copy(owner).start()

    @pl.loop(1, slots // group)
    def _(turn):
        batch = [turn * group + at for at in range(group)]
        for slot in batch:
            x_copy(slot).wait()
            a_copy(slot).wait()
        for slot, root in compute(batch, [a_buf[slot - group] for slot in batch], [x_buf[slot - group] for slot in batch]):
            high[core, slot - group] = root
        for slot in batch:
            p_copy(core, slot).start()

    def launch(position, filled, early=False, taken=None):
        at_core, at_slot = packed_at(kept_index(position - filled, mine.excess), mine.first, mine.second, slots)
        value = low[at_core, jnp.minimum(at_slot, group - 1), rows_of(core)]
        if not early:
            later = high[at_core, jnp.maximum(at_slot - group, 0), rows_of(core)]
            value = lax.select_n(at_slot >= group, value, later)
        if taken is not None:
            value = lax.select_n(taken < theirs.excess, value, relayed[taken])
        staged[position - 2] = value
        for offset in range(1, chips):
            y_copy(offset, position).start()

    def near_apply(which):
        for at in range(group):
            near[which, at] = dot(low[which, at], g_buf[2 * chip + which, at]).astype(near.dtype)

        @pl.loop(1, slots // group)
        def _(turn):
            for at in range(group):
                slot = turn * group + at
                near[which, slot] = dot(high[which, slot - group], g_buf[2 * chip + which, slot]).astype(near.dtype)

    def receive(early):
        @pl.loop(0 if early else group, group if early else slots)
        def _(slot):
            p_copy(other, slot, early).wait_recv()

    receive(True)
    for position in range(2, window):
        launch(position, 0, True)
    for number in range(relays):
        position = window + number
        if position == min(group + 1, window + relays - 1):
            for owner in range(members):
                g_copy(owner).wait()
            near_apply(core)
            receive(False)
        relay_copy(number, core).wait_recv()
        launch(position, theirs.excess, position <= group, number)

    @pl.loop(window + relays, capacity(positions, spared, chip, data))
    def _(position):
        launch(position, theirs.excess)

    near_apply(other)
    last = far.shape[1] - 1
    for at in range(chips - 1):
        far[at, last] = jnp.zeros(far.shape[2:], far.dtype)

    loads = {offset: [Load(counts, source_of(offset), at, positions, spared) for at in (data, beside)]
             for offset in range(1, chips)}

    def arrive(offset, kind, number):
        if kind == "first":
            first_copy(offset).wait_recv()
            first_forward(offset, core).start()
        elif kind == "position":
            y_copy(offset, number).wait_recv()
            forward(offset, number, core).start()
            if window <= number < window + relays:
                back_copy(offset, number - window).start()
        else:
            back_copy(offset, number).wait_recv()
            back_forward(offset, number, core).start()

    def apply(offset, kind, number):
        source = source_of(offset)
        at = offset - 1
        if kind == "first":
            first_forward(offset, other).wait_recv()
            for which in range(2):
                far[at, which] = dot(landed[at, which], g_buf[2 * source + which, 0]).astype(far.dtype)
        elif kind == "position":
            forward(offset, number, other).wait_recv()
            own, side = loads[offset]
            index = kept_index(number - side.excess if number >= window else number, own.excess)
            at_core, at_slot = packed_at(index, own.first, own.second, slots)
            far[at, number] = dot(landed[at, number], g_buf[2 * source + at_core, at_slot]).astype(far.dtype)
        else:
            back_forward(offset, number, other).wait_recv()
            at_core, at_slot = relayed_block(number)
            far[at, positions + number] = dot(returned[at, number], g_buf[2 * source + at_core, at_slot]).astype(far.dtype)

    events = [(2.0, "first", 0)]
    events += [(position + 1.0, "position", position) for position in range(2, positions)]
    events += [(window + number + BACK, "back", number) for number in range(relays)]
    events = [event[1:] for event in sorted(events)]
    def where_sent(sender, position):
        if position < positions - sum(spared):
            return lambda run: run()
        return pl.when(position < capacity(positions, spared, sender, data))

    def at_each_offset(step, kind, number):
        for offset in range(1, chips):
            when = where_sent(source_of(offset), number) if kind == "position" else (lambda run: run())
            when(functools.partial(step, offset, kind, number))

    at_each_offset(arrive, *events[0])
    for before, now in zip(events, events[1:]):
        at_each_offset(arrive, *now)
        at_each_offset(apply, *before)

    @pl.loop(0, group)
    def _(slot):
        p_copy(core, slot, True).wait_send()

    @pl.loop(group, slots)
    def _(slot):
        p_copy(core, slot).wait_send()

    for number in range(relays):
        @pl.when(core == relayed_block(number)[0])
        def _():
            for which in range(2):
                relay_copy(number, which).wait_send()

    def sent(offset, kind, number):
        if kind == "first":
            first_copy(offset).wait_send()
        elif kind == "position":
            y_copy(offset, number).wait_send()
        else:
            back_copy(offset, number).wait_send()

    def forwarded(offset, kind, number):
        if kind == "first":
            first_forward(offset, core).wait_send()
        elif kind == "position":
            forward(offset, number, core).wait_send()
        else:
            back_forward(offset, number, core).wait_send()

    for kind, number in events:
        for offset in range(1, chips):
            when = where_sent(chip, number) if kind == "position" else (lambda run: run())
            when(functools.partial(sent, offset, kind, number))
    for event in events[:-1]:
        at_each_offset(forwarded, *event)
    at_each_offset(apply, *events[-1])
    at_each_offset(forwarded, *events[-1])


def placing_kernel(members, positions, spared, relays, window, counts, near, far, out, near_sem, far_sem):
    me = lax.axis_index("mp")
    data = lax.axis_index("dp")
    chips = members // 2
    chip = me // 2
    slots = near.shape[1]

    def near_copy(which):
        return pltpu.make_async_copy(near.at[which], out.at[2 * chip + which], near_sem.at[which])

    for which in range(2):
        near_copy(which).start()
    copies = []
    for offset in range(1, chips):
        source = lax.rem(chip + chips - offset, chips)
        own, side = (Load(counts, source, at, positions, spared) for at in (data, neighbour_of(data)))
        both = jnp.minimum(own.first, own.second)
        for which in range(2):
            for slot in range(slots):
                index = jnp.where(slot < both, 2 * slot + which, slot + both)
                odd = lax.rem(index, 2)
                near_start = index <= 2 * own.excess + 1
                kept = jnp.where(index < 2, index, jnp.where(near_start, lax.div(index + 1, 2), index - own.excess))
                place = jnp.where(kept < window, kept, kept + side.excess)
                passed = (index >= 2) & near_start & (odd == 0)
                place = jnp.where(passed, positions + lax.div(index, 2) - 1, place)
                place = jnp.where(slot < (own.first, own.second)[which], place, far.shape[1] - 1)
                copies.append(pltpu.make_async_copy(
                    far.at[offset - 1, place], out.at[2 * source + which, slot], far_sem.at[offset - 1, which, slot]))
                copies[-1].start()
    for which in range(2):
        near_copy(which).wait()
    for copy in copies:
        copy.wait()


def exchange(members, number, positions, spared, relays, window, counts, first_a, first_x, stats, prev_roots, grads):
    slots, size = stats.shape[1], stats.shape[2]
    chips = members // 2
    square = (size, size)
    near = (2, slots) + square
    far = (chips - 1, positions + relays + 1) + square
    group = first_a.shape[0]
    kept = grads.dtype.itemsize * size * size * (near[0] * near[1] + far[0] * far[1])
    kept += 2 * first_a.size * first_a.dtype.itemsize
    semaphores = pltpu.SemaphoreType.DMA
    steps, backs = (chips - 1, positions - 1), (chips - 1, relays)
    near, far = pl.pallas_call(
        functools.partial(kernel, members, positions, spared, relays, window),
        out_shape=(pltpu.VMEM(near, grads.dtype), pltpu.VMEM(far, grads.dtype)),
        in_specs=[pl.BlockSpec(memory_space=space)
                  for space in (pltpu.SMEM, pltpu.VMEM, pltpu.VMEM, pltpu.HBM, pltpu.HBM, pltpu.HBM)],
        out_specs=(pl.BlockSpec(memory_space=pltpu.VMEM), pl.BlockSpec(memory_space=pltpu.VMEM)),
        scratch_shapes=[
            pltpu.VMEM((slots - group,) + square, jnp.float32),
            pltpu.VMEM((slots - group,) + square, jnp.float32),
            pltpu.VMEM(grads.shape, grads.dtype),
            pltpu.VMEM((2, group) + square, jnp.bfloat16),
            pltpu.VMEM((2, slots - group) + square, jnp.bfloat16),
            pltpu.VMEM((positions - 2, size // 2, size), jnp.bfloat16),
            pltpu.VMEM((chips - 1, positions) + square, jnp.bfloat16),
            pltpu.VMEM((relays, size // 2, size), jnp.bfloat16),
            pltpu.VMEM((chips - 1, relays) + square, jnp.bfloat16),
            semaphores((slots - group,)),
            semaphores((slots - group,)),
            semaphores((members,)),
            semaphores(steps),
            semaphores(steps),
            semaphores((slots,)),
            semaphores((slots,)),
            semaphores(steps),
            semaphores(steps),
            semaphores((relays, 2)),
            semaphores((relays,)),
            semaphores(backs),
            semaphores(backs),
            semaphores(backs),
            semaphores(backs),
        ],
        compiler_params=pltpu.CompilerParams(
            collective_id=number, has_side_effects=True, vmem_limit_bytes=VMEM_BYTES - kept),
    )(counts, first_a, first_x, stats, prev_roots, grads)
    return pl.pallas_call(
        functools.partial(placing_kernel, members, positions, spared, relays, window),
        out_shape=pltpu.HBM(grads.shape, grads.dtype),
        in_specs=[
            pl.BlockSpec(memory_space=pltpu.SMEM),
            pl.BlockSpec(memory_space=pltpu.VMEM),
            pl.BlockSpec(memory_space=pltpu.VMEM),
        ],
        out_specs=pl.BlockSpec(memory_space=pltpu.HBM),
        scratch_shapes=[
            semaphores((2,)),
            semaphores((chips - 1, 2, slots)),
        ],
        compiler_params=pltpu.CompilerParams(vmem_limit_bytes=1 << 20),
    )(counts, near, far)


def local(members, stats, prev_roots, counts, grads):
    slots = stats.shape[1]
    variants = [(slots + 2, (1, 1), RELAYS - 1)]
    variants += [(size, (0, 1), RELAYS) for size in range(slots + 2, slots + 5)]
    variants += [(2 * slots, (0, 0), RELAYS)]
    first = (GROUP,) + stats.shape[2:]
    semaphores = pltpu.SemaphoreType.DMA
    choice, table, first_a, first_x = pl.pallas_call(
        functools.partial(opening_kernel, variants, slots),
        out_shape=(pltpu.SMEM((1,), jnp.int32), pltpu.SMEM(counts.shape, counts.dtype),
                   pltpu.VMEM(first, stats.dtype), pltpu.VMEM(first, stats.dtype)),
        in_specs=[pl.BlockSpec(memory_space=pltpu.HBM)] * 3,
        out_specs=tuple(pl.BlockSpec(memory_space=space) for space in (pltpu.SMEM, pltpu.SMEM, pltpu.VMEM, pltpu.VMEM)),
        scratch_shapes=[semaphores, semaphores((GROUP,)), semaphores((GROUP,))],
        compiler_params=pltpu.CompilerParams(vmem_limit_bytes=1 << 20),
    )(pltpu.with_memory_space_constraint(counts, pltpu.HBM), stats, prev_roots)
    branches = [functools.partial(exchange, members, number, *variant, WINDOW) for number, variant in enumerate(variants)]
    return lax.switch(choice[0], branches, table, first_a, first_x, stats, prev_roots, grads)


def solution(mesh):
    return jax.shard_map(
        functools.partial(local, mesh.shape["mp"]),
        mesh=mesh,
        in_specs=(
            P("mp", "dp", None, None),
            P("mp", "dp", None, None),
            P(),
            P(None, "dp", None, "mp"),
        ),
        out_specs=P(None, "dp", None, "mp"),
        check_vma=False,
    )
```
